128 devices in a mesh: expert: 16 (over z, x), tensor: 8 (over y, core).
Axes of the slice: x: 4, y: 4, z: 4, core: 2. Of those that a mesh axis runs over, the one named last changes fastest.
Arguments:
- tokens: bfloat16 [2048, 4096], P('expert'), may hold values from -6 to 6
- scores: float32 [2048, 8], P('expert'), may hold values from -6 to 6
- expert_ids: int32 [2048, 8], P('expert'), may hold values from 0 to 63, all different within a row; in each aligned block of 128 rows (0 to 127, 128 to 255, ...) at most 32 rows name the same one
- gate_weight: bfloat16 [64, 1536, 4096], P('expert', 'tensor'), may hold values from -0.09375 to 0.09375
- up_weight: bfloat16 [64, 1536, 4096], P('expert', 'tensor'), may hold values from -0.09375 to 0.09375
- down_weight: bfloat16 [64, 1536, 4096], P('expert', 'tensor'), may hold values from -0.15625 to 0.15625
Outputs:
- mixed: bfloat16 [2048, 4096], P('expert', 'tensor')
The draws below stay inside these ranges and needn't reach their ends.
Inputs may be any that keep to these rules, and one draw needn't show every extreme that they name: `expert_ids`: each row names 8 different experts. Among the 128 rows of one owner (rows o * 128 to (o + 1) * 128 - 1) no expert is named more than 32 times.
All inputs are finite; a program needn't handle non-finite values.
Results may differ from the reference program's by a relative error of at most 0.018.
Values may be sent and summed in bfloat16 or wider, within the bound.
A program may use at most 128 MiB of HBM per device.

```python
import math
import jax
import jax.numpy as jnp
import numpy as np
from jax import lax

D = 4096
FF = 1536
TOP = 8
EXP_DEV = 4
TOK_DEV = 128
EXPERTS = 64
TOKENS = 2048
M = 32
N_EXPERT = 16
N_TENSOR = 8


def block_scale(key, extent, shards, least, top_value):
    gain = 1.0
    for dim, shards_of in shards:
        heights = jax.random.uniform(jax.random.fold_in(jax.random.fold_in(key, 6), dim), (shards_of,), jnp.float32, least / len(shards), top_value / len(shards))
        gain = gain * jnp.repeat(jnp.exp(heights), extent[dim] // shards_of).reshape((-1,) + (1,) * (len(extent) - 1 - dim))
    return gain


def assign_block(key, own, number, rows, amount, top, bound, skew):
    sequence = jax.random.permutation(key, amount)
    heavy_load, ordinary = load_shares(amount, rows * top, bound, skew, True), load_shares(amount, rows * top, bound, skew, False)
    places = jnp.arange(amount)

    def named(tallies, rotation):
        used = int((tallies > 0).sum())
        fixed = max(1, used // 4)
        moved = fixed + (places - fixed + rotation * (used - fixed)) % max(1, amount - fixed)
        return jnp.zeros((amount,), jnp.int32).at[sequence[jnp.where(places < fixed, places, moved)]].set(jnp.asarray(tallies, jnp.int32))

    tallies = jnp.where(number % 4 == 0, named(heavy_load, number // 4), named(ordinary, number - number // 4 - 1))
    mixed = jax.random.permutation(jax.random.fold_in(own, 3), amount)
    source_of, taker = mixed[0:amount // 2 * 2:2], mixed[1:amount // 2 * 2:2]
    margin = jnp.minimum(tallies[source_of] - 1, bound - tallies[taker]) // 2
    margin = jnp.where((source_of == sequence[0]) | (taker == sequence[0]) | (tallies[taker] == 0), 0, jnp.maximum(margin, 0))
    moved = jax.random.randint(jax.random.fold_in(own, 4), (amount // 2,), 0, 1 << 20) % (margin + 1)
    tallies = tallies.at[source_of].add(-moved).at[taker].add(moved)
    items = jnp.searchsorted(jnp.cumsum(tallies), jnp.arange(rows * top), side="right").astype(jnp.int32)
    listing = items.reshape(top, rows).T
    listing = listing[jax.random.permutation(jax.random.fold_in(own, 1), rows)]
    rotation = jax.random.randint(jax.random.fold_in(own, 2), (rows, 1), 0, top)
    return jnp.take_along_axis(listing, (jnp.arange(top)[None, :] + rotation) % top, axis=1)


def load_shares(amount, total, most, slope, full):
    weights = [(1 << 20) // math.isqrt(standing ** slope) + 1 for standing in range(1, amount + 1)]
    largest = most if full else min(most, max(-(-total // amount), total * weights[0] // sum(weights)))
    least = 1 if total - largest >= amount - 1 else 0
    given, spare = [largest] + [least] * (amount - 1), total - largest - least * (amount - 1)
    while spare > 0:
        candidates = [i for i in range(1, amount) if given[i] < largest] or [i for i in range(1, amount) if given[i] < most]
        pool, left = sum([weights[i] for i in candidates]), spare
        for i in candidates:
            extra = min(most - given[i], max(1, left * weights[i] // pool), spare)
            given[i] = given[i] + extra
            spare = spare - extra
    return np.array(given)


def scatter_about(key, dims, deviation, bound, shards=(), kind=jnp.bfloat16):
    values = jax.random.normal(key, dims, jnp.float32) * deviation
    if len(shards) > 0:
        values = block_scale(key, dims, shards, -0.22, 0.18) * values
    return jnp.clip(values, min=-bound, max=bound).astype(kind)


def setup_inputs(seed: int = 0) -> dict:
    seeds = jax.random.split(jax.random.key(seed), 7)
    tokens = scatter_about(seeds[0], (TOKENS, D), 1.0, 6.0, ((0, 16),))
    scores = scatter_about(seeds[1], (TOKENS, TOP), 1.0, 6.0, ((0, 16),), jnp.float32)
    expert_ids_keys = jax.random.split(jax.random.fold_in(seeds[2], 1), TOKENS // TOK_DEV)
    expert_ids_turns = jax.random.permutation(jax.random.fold_in(seeds[2], 3), TOKENS // TOK_DEV)
    expert_ids = jax.vmap(lambda own, number: assign_block(jax.random.fold_in(seeds[2], 2), own, number, TOK_DEV, EXPERTS, TOP, M, 1))(expert_ids_keys, expert_ids_turns).reshape((TOKENS, TOP))
    gate_weight = scatter_about(seeds[3], (EXPERTS, FF, D), D ** -0.5, 0.09375, ((0, 16), (1, 8)))
    up_weight = scatter_about(seeds[4], (EXPERTS, FF, D), D ** -0.5, 0.09375, ((0, 16), (1, 8)))
    down_weight = scatter_about(seeds[5], (EXPERTS, FF, D), FF ** -0.5, 0.15625, ((0, 16), (1, 8)))
    return {"tokens": tokens, "scores": scores, "expert_ids": expert_ids, "gate_weight": gate_weight, "up_weight": up_weight, "down_weight": down_weight}


def gate_of(scores):
    lifted = jnp.exp(scores.astype(jnp.float32))
    return (lifted / jnp.sum(lifted, axis=-1, keepdims=True)).astype(jnp.bfloat16)


def slot_tables(expert_ids, gate_values, experts, blocks, capacity):
    rows_all = expert_ids.shape[0]
    block_rows = rows_all // blocks
    expert_count = experts.shape[0]
    matches = expert_ids[:, :, None] == experts[None, None, :]
    routed = jnp.any(matches, axis=1).astype(jnp.int32)
    chosen_gate = jnp.sum(jnp.where(matches, gate_values.astype(jnp.float32)[:, :, None], jnp.float32(0.0)), axis=1)
    folded = routed.reshape(blocks, block_rows, expert_count)
    rank_in_block = (jnp.cumsum(folded, axis=1) - folded).astype(jnp.int32)
    block_start = (jnp.arange(blocks, dtype=jnp.int32) * capacity)[:, None, None]
    slot_index = (block_start + rank_in_block).reshape(rows_all, expert_count).astype(jnp.int32)
    slot_index = jnp.where(routed == 1, slot_index, blocks * capacity).astype(jnp.int32)
    columns = jnp.broadcast_to(jnp.arange(expert_count, dtype=jnp.int32)[None, :], slot_index.shape)
    position = jnp.broadcast_to(jnp.arange(rows_all, dtype=jnp.int32)[:, None], slot_index.shape)
    slot_token = jnp.full((expert_count, blocks * capacity), rows_all, jnp.int32).at[columns, slot_index].set(position, mode="drop")
    slot_gate = jnp.zeros((expert_count, blocks * capacity), jnp.float32).at[columns, slot_index].set(chosen_gate, mode="drop")
    return slot_token, slot_gate


def reference(tokens, scores, expert_ids, gate_weight, up_weight, down_weight):
    gate_values = gate_of(scores)
    experts = jnp.arange(EXP_DEV * N_EXPERT, dtype=jnp.int32)
    slot_token, slot_gate = slot_tables(expert_ids, gate_values, experts, N_EXPERT, M)
    share = FF // N_TENSOR

    def one_expert(total, inputs):
        token_index, gate_column, w_gate, w_up, w_down = inputs
        rows = jnp.take(tokens, token_index, axis=0, mode="fill", fill_value=0)
        gate = jnp.dot(rows, w_gate.T, preferred_element_type=jnp.float32)
        upward = jnp.dot(rows, w_up.T, preferred_element_type=jnp.float32)
        hidden = (jax.nn.silu(gate) * upward).astype(jnp.bfloat16)
        pieces = hidden.reshape(hidden.shape[0], N_TENSOR, share).astype(jnp.float32)
        blocks_down = w_down.reshape(N_TENSOR, share, D).astype(jnp.float32)
        partial_value = jnp.einsum("cnf,nfd->ncd", pieces, blocks_down).astype(jnp.bfloat16)
        summed = jnp.sum(partial_value.astype(jnp.float32), axis=0)
        gated = summed * gate_column[:, None]
        total = total.at[token_index].add(gated, mode="drop")
        return total, jnp.float32(0.0)

    start = jnp.zeros((tokens.shape[0], D), jnp.float32)
    total = lax.scan(one_expert, start, (slot_token, slot_gate, gate_weight, up_weight, down_weight))[0]
    return total.astype(jnp.bfloat16)
```

```python
import jax
import jax.numpy as jnp
from jax import lax
from jax.experimental import pallas as pl
from jax.experimental.pallas import tpu as pltpu
from jax.sharding import PartitionSpec as P

MESH = pl.DeviceIdType.MESH
f32 = jnp.float32
bf16 = jnp.bfloat16

RING = 4
OWN = 128
WIDTH = 4096
FFS = 192
HELD = 4
CAP = 32
QUART = 1024
INFO = 16
CHUNK = 512
BATCH = RING * OWN
ORDER = (2, 1, 3, 0)
NT = (((1,), (1,)), ((), ()))


def distance(kind, dz, dx):
    if kind == 0:
        return dx if dz == 0 else dz
    return dz if dx == 0 else dx


def transfer_ids():
    ids = {}
    for kind in range(2):
        for dz in range(RING):
            for dx in range(RING):
                if dz == 0 and dx == 0:
                    continue
                parts = ("h0", "h1") if distance(kind, dz, dx) == 2 else ("f",)
                for part in parts:
                    ids[kind, dz, dx, part] = len(ids)
                ids[kind, dz, dx, "d"] = len(ids)
    return ids


IDS = transfer_ids()


def kernel(
    tokens, info, wg_in, wu_in, wd_in, out,
    xa, xb, wg, wu, wd, rows, pmat, pgt, hid, part_buf, mine, theirs, dgot,
    y1got, y2got, tot, x1got, x2got, kept, leaving, zgot,
    lsem, ssem, rsem, d_s, d_r, y_s, y_r, x_s, x_r, z_s, z_r,
):
    me = lax.axis_index("expert")
    rank = lax.axis_index("tensor")
    z, x = me // RING, me % RING
    y, c = rank // 2, rank % 2
    other = 1 - c

    def device(dz, dx, dy, core):
        return (((z + dz) % RING) * RING + (x + dx) % RING, ((y + dy) % RING) * 2 + core)

    peers = [
        device(0, 1, 0, c), device(0, 3, 0, c), device(1, 0, 0, c), device(3, 0, 0, c),
        device(2, 0, 0, c), device(0, 0, 1, c), device(0, 0, 3, c), device(0, 0, 0, other),
    ]
    barrier = pltpu.get_barrier_semaphore()
    for peer in peers:
        pl.semaphore_signal(barrier, inc=1, device_id=peer, device_id_type=MESH)

    bufs = (xa, xb)
    loads = []

    def load(src, dst):
        copy = pltpu.make_async_copy(src, dst, lsem.at[len(loads)])
        loads.append(copy)
        copy.start()
        return copy

    own_loads = []
    for half in range(2):
        own_loads.append(load(tokens.at[:, pl.ds(half * 2048, QUART)], xa.at[half, me, pl.ds(0, OWN)]))
        own_loads.append(load(info, xa.at[half, me, pl.ds(OWN, INFO)]))
        own_loads.append(load(tokens.at[:, pl.ds(half * 2048 + QUART, QUART)], xb.at[half, me]))
    weight_loads = [load(wg_in, wg), load(wu_in, wu), load(wd_in, wd)]

    def view(kind, half, dz, dx, part):
        owner = ((z + dz) % RING) * RING + (x + dx) % RING
        buf = bufs[kind]
        if part == "h0":
            return buf.at[half, owner, pl.ds(0, 64)]
        if part == "h1":
            return buf.at[half, owner, pl.ds(64, buf.shape[2] - 64)]
        return buf.at[half, owner]

    started = {}

    def describe(kind, dz, dx, part, tz, tx):
        ident = IDS[kind, (dz - tz) % RING, (dx - tx) % RING, part]
        ref = view(kind, c, dz, dx, part)
        return pltpu.make_async_remote_copy(
            src_ref=ref, dst_ref=ref, send_sem=ssem.at[ident], recv_sem=rsem.at[ident],
            device_id=device(tz, tx, 0, c), device_id_type=MESH,
        )

    def send(kind, dz, dx, part, tz, tx):
        started[describe, (kind, dz, dx, part, tz, tx)] = True
        describe(kind, dz, dx, part, tz, tx).start()

    def describe_pair(kind, dz, dx, half=c):
        ident = IDS[kind, dz, dx, "d"]
        ref = view(kind, half, dz, dx, "f")
        return pltpu.make_async_remote_copy(
            src_ref=ref, dst_ref=ref, send_sem=ssem.at[ident], recv_sem=rsem.at[ident],
            device_id=device(0, 0, 0, other), device_id_type=MESH,
        )

    def pair(kind, dz, dx):
        started[describe_pair, (kind, dz, dx)] = True
        describe_pair(kind, dz, dx).start()

    def got_pair(kind, dz, dx):
        describe_pair(kind, dz, dx, other).wait_recv()

    def got(kind, dz, dx, part):
        ident = IDS[kind, dz, dx, part]
        ref = view(kind, c, dz, dx, part)
        pltpu.make_async_remote_copy(
            src_ref=ref, dst_ref=ref, send_sem=ssem.at[ident], recv_sem=rsem.at[ident],
            device_id=device(0, 0, 0, other), device_id_type=MESH,
        ).wait_recv()

    def along(kind, first, step):
        if (kind == 0) == first:
            return (0, step)
        return (step, 0)

    def arrive(kind, first, dz, dx):
        d = distance(kind, dz, dx)
        if d == 2:
            got(kind, dz, dx, "h0")
            got(kind, dz, dx, "h1")
        else:
            got(kind, dz, dx, "f")
            if d == 3:
                send(kind, dz, dx, "h0", *along(kind, first, 1))
            else:
                send(kind, dz, dx, "h1", *along(kind, first, 3))
        pair(kind, dz, dx)

    def spread(kind, first, dz, dx):
        for step in (1, 3):
            send(kind, dz, dx, "f", *along(kind, first, step))

    pl.semaphore_wait(barrier, len(peers))
    for copy in own_loads:
        copy.wait()
    spread(0, True, 0, 0)
    spread(1, True, 0, 0)
    spread(1, False, 0, 0)
    spread(0, False, 0, 0)
    for copy in weight_loads:
        copy.wait()

    arrive(0, True, 0, 3)
    arrive(0, True, 0, 1)
    arrive(1, True, 3, 0)
    arrive(1, True, 1, 0)
    arrive(1, False, 0, 3)
    arrive(1, False, 0, 1)
    spread(1, False, 1, 0)
    spread(1, False, 3, 0)
    spread(0, False, 0, 3)
    spread(0, False, 0, 1)
    arrive(0, True, 0, 2)
    spread(0, False, 0, 2)
    arrive(1, False, 0, 2)
    arrive(0, False, 1, 0)
    arrive(0, False, 3, 0)
    arrive(1, True, 2, 0)
    spread(1, False, 2, 0)

    def arrive_rest(dz):
        for dx in (3, 1):
            arrive(0, False, dz, dx)
            arrive(1, False, dz, dx)
        if dz == 2:
            arrive(0, False, 2, 0)
        arrive(0, False, dz, 2)
        arrive(1, False, dz, 2)

    def batch_z(b):
        return (b * (b + 1) // 2) % RING

    def slots(zz):
        earlier = lax.broadcasted_iota(jnp.int32, (OWN, OWN), 0)
        later = lax.broadcasted_iota(jnp.int32, (OWN, OWN), 1)
        triangle = jnp.where(earlier < later, 1.0, 0.0).astype(bf16)
        routed, gates = [], []
        for o in range(RING):
            facts = xa[0, zz * RING + o, pl.ds(OWN, INFO), pl.ds(0, OWN)].astype(f32)
            named, values = facts[0:8], facts[8:16]
            for j in range(HELD):
                match = named == (me * HELD + j).astype(f32)
                routed.append(jnp.max(jnp.where(match, 1.0, 0.0), axis=0, keepdims=True))
                gates.append(jnp.sum(jnp.where(match, values, 0.0), axis=0, keepdims=True))
        chosen = jnp.concatenate(routed, axis=0)
        place = jnp.dot(chosen.astype(bf16), triangle, preferred_element_type=f32)
        slot = lax.broadcasted_iota(jnp.int32, (CAP, OWN), 0).astype(f32)
        for o in range(RING):
            gated = []
            for j in range(HELD):
                i = o * HELD + j
                hit = jnp.where(slot == place[i : i + 1], 1.0, 0.0) * routed[i]
                pmat[o, pl.ds(j * CAP, CAP)] = hit.astype(bf16)
                gated.append(hit * gates[i])
            pgt[o] = jnp.concatenate(gated, axis=0).T.astype(bf16)

    def gather(zz):
        def one(o, carry):
            pick = pmat[o]
            for half in range(2):
                for kind in range(2):
                    block = bufs[kind][half, zz * RING + o, pl.ds(0, OWN)]
                    taken = jnp.dot(pick, block, preferred_element_type=f32).astype(bf16)
                    for e in range(HELD):
                        rows[e, pl.ds(o * CAP, CAP), pl.ds(half * 2048 + kind * QUART, QUART)] = taken[
                            e * CAP : (e + 1) * CAP
                        ]
            return carry

        lax.fori_loop(0, RING, one, 0)

    def experts():
        def one(e, carry):
            held = rows[e]
            gate = lax.dot_general(held, wg[e], NT, preferred_element_type=f32)
            up = lax.dot_general(held, wu[e], NT, preferred_element_type=f32)
            hid[e] = (gate * (1.0 / (1.0 + jnp.exp(-gate))) * up).astype(bf16)
            return carry

        lax.fori_loop(0, HELD, one, 0)

    def down(s, i, block, dst):
        column = pl.multiple_of(block * CHUNK, CHUNK)
        for e in range(HELD):
            value = jnp.dot(hid[e], wd[e, :, pl.ds(column, CHUNK)], preferred_element_type=f32).astype(bf16)
            for o in range(RING):
                part_buf[o, pl.ds(e * CAP, CAP)] = value[o * CAP : (o + 1) * CAP]
        for o in range(RING):
            dst[s, i, pl.ds(o * OWN, OWN)] = jnp.dot(
                pgt[o], part_buf[o], preferred_element_type=f32
            ).astype(bf16)

    def d_copy(s, i):
        return pltpu.make_async_remote_copy(
            src_ref=theirs.at[s, i], dst_ref=dgot.at[s, i], send_sem=d_s.at[s, i], recv_sem=d_r.at[s, i],
            device_id=device(0, 0, 0, other), device_id_type=MESH,
        )

    def y_copies(s, stage):
        if stage == 0:
            pieces = ((mine.at[s, 0, pl.ds(0, 256)], y1got.at[s, 0]), (mine.at[s, 0, pl.ds(256, 256)], y1got.at[s, 1]))
        else:
            pieces = ((mine.at[s, 1], y2got.at[s, 0]), (mine.at[s, 2], y2got.at[s, 1]))
        return [
            pltpu.make_async_remote_copy(
                src_ref=src, dst_ref=dst, send_sem=y_s.at[s, stage * 2 + n], recv_sem=y_r.at[s, stage * 2 + n],
                device_id=device(0, 0, (1, 3)[n], c), device_id_type=MESH,
            )
            for n, (src, dst) in enumerate(pieces)
        ]

    def owner_rows(dx, start, size):
        return pl.ds(pl.multiple_of(((x + dx) % RING) * OWN + start, 64), size)

    def x_copies(s, stage):
        if stage == 0:
            pieces = (
                (tot.at[s, owner_rows(2, 0, 64)], x1got.at[s, 0]),
                (tot.at[s, owner_rows(2, 64, 64)], x1got.at[s, 1]),
            )
        else:
            pieces = ((tot.at[s, owner_rows(1, 0, OWN)], x2got.at[s, 0]), (tot.at[s, owner_rows(3, 0, OWN)], x2got.at[s, 1]))
        return [
            pltpu.make_async_remote_copy(
                src_ref=src, dst_ref=dst, send_sem=x_s.at[s, stage * 2 + n], recv_sem=x_r.at[s, stage * 2 + n],
                device_id=device(0, (1, 3)[n], 0, c), device_id_type=MESH,
            )
            for n, (src, dst) in enumerate(pieces)
        ]

    def z_copy(i):
        b = i + 1
        return pltpu.make_async_remote_copy(
            src_ref=leaving.at[i], dst_ref=zgot.at[i], send_sem=z_s.at[i], recv_sem=z_r.at[i],
            device_id=device(batch_z(b), 0, 0, c), device_id_type=MESH,
        )

    def backs(s):
        for i, r in enumerate(ORDER):
            base = ((y + r) % RING) * 2
            down(s, i, base + other, theirs)
            d_copy(s, i).start()
            down(s, i, base + c, mine)
            d_copy(s, i).wait()
            mine[s, i] = (mine[s, i].astype(f32) + dgot[s, i].astype(f32)).astype(bf16)
            if i == 0:
                for copy in y_copies(s, 0):
                    copy.start()

    def y_second(s):
        for copy in y_copies(s, 0):
            copy.wait()
        lo, hi = pl.ds(0, 256), pl.ds(256, 256)
        mine[s, 1, lo] = (mine[s, 1, lo].astype(f32) + y1got[s, 0].astype(f32)).astype(bf16)
        mine[s, 2, hi] = (mine[s, 2, hi].astype(f32) + y1got[s, 1].astype(f32)).astype(bf16)
        for copy in y_copies(s, 1):
            copy.start()

    def y_third(s):
        for copy in y_copies(s, 1):
            copy.wait()
        tot[s] = (mine[s, 3].astype(f32) + y2got[s, 0].astype(f32) + y2got[s, 1].astype(f32)).astype(bf16)
        for copy in x_copies(s, 0):
            copy.start()

    def x_second(s):
        for copy in x_copies(s, 0):
            copy.wait()
        lo, hi = owner_rows(1, 0, 64), owner_rows(3, 64, 64)
        tot[s, lo] = (tot[s, lo].astype(f32) + x1got[s, 0].astype(f32)).astype(bf16)
        tot[s, hi] = (tot[s, hi].astype(f32) + x1got[s, 1].astype(f32)).astype(bf16)
        for copy in x_copies(s, 1):
            copy.start()

    def x_third(b, s):
        for copy in x_copies(s, 1):
            copy.wait()
        value = tot[s, owner_rows(0, 0, OWN)].astype(f32) + x2got[s, 0].astype(f32) + x2got[s, 1].astype(f32)

        @pl.when(b == 0)
        def _():
            kept[...] = value

        @pl.when(b > 0)
        def _():
            leaving[b - 1] = value.astype(bf16)
            z_copy(b - 1).start()

    def batch(b, carry):
        s = b % 2
        before = (b + 1) % 2
        dz = batch_z(b)
        zz = (z + dz) % RING
        for value in range(1, RING):
            step = batch_z(value)

            @pl.when(b == value)
            def _():
                if value == 1:
                    arrive_rest(1)
                    arrive_rest(3)
                if value == 3:
                    arrive_rest(2)
                for dx in range(RING):
                    got_pair(0, step, dx)
                    got_pair(1, step, dx)

        @pl.when(b == 0)
        def _():
            for dx in range(1, RING):
                got_pair(0, 0, dx)
                got_pair(1, 0, dx)

        slots(zz)
        gather(zz)

        @pl.when(b > 0)
        def _():
            y_second(before)

        experts()

        @pl.when(b > 1)
        def _():
            x_third(b - 2, s)

        backs(s)

        @pl.when(b > 0)
        def _():
            y_third(before)
            x_second(before)

        return carry

    lax.fori_loop(0, RING, batch, 0)
    y_second(1)
    x_third(2, 0)
    y_third(1)
    x_second(1)
    x_third(3, 1)
    total = kept[...]
    for i in range(3):
        z_copy(i).wait()
        total = total + zgot[i].astype(f32)
    out[...] = total.astype(bf16)
    for describe_one, args in started:
        describe_one(*args).wait_send()


def gate_of(scores):
    lifted = jnp.exp(scores)
    return (lifted / jnp.sum(lifted, axis=-1, keepdims=True)).astype(bf16)


def local(tokens, scores, expert_ids, gate_weight, up_weight, down_weight):
    info = jnp.concatenate([expert_ids.astype(bf16).T, gate_of(scores).T], axis=0)
    info = jnp.pad(info, ((0, 0), (0, QUART - OWN)))
    dma = pltpu.SemaphoreType.DMA
    count = len(IDS)
    return pl.pallas_call(
        kernel,
        out_shape=jax.ShapeDtypeStruct((OWN, CHUNK), bf16),
        in_specs=[pl.BlockSpec(memory_space=pl.ANY)] * 5,
        out_specs=pl.BlockSpec(memory_space=pltpu.VMEM),
        scratch_shapes=[
            pltpu.VMEM((2, 16, OWN + INFO, QUART), bf16),
            pltpu.VMEM((2, 16, OWN, QUART), bf16),
            pltpu.VMEM((HELD, FFS, WIDTH), bf16),
            pltpu.VMEM((HELD, FFS, WIDTH), bf16),
            pltpu.VMEM((HELD, FFS, WIDTH), bf16),
            pltpu.VMEM((HELD, OWN, WIDTH), bf16),
            pltpu.VMEM((RING, OWN, OWN), bf16),
            pltpu.VMEM((RING, OWN, OWN), bf16),
            pltpu.VMEM((HELD, OWN, FFS), bf16),
            pltpu.VMEM((RING, OWN, CHUNK), bf16),
            pltpu.VMEM((2, 4, BATCH, CHUNK), bf16),
            pltpu.VMEM((2, 4, BATCH, CHUNK), bf16),
            pltpu.VMEM((2, 4, BATCH, CHUNK), bf16),
            pltpu.VMEM((2, 2, BATCH // 2, CHUNK), bf16),
            pltpu.VMEM((2, 2, BATCH, CHUNK), bf16),
            pltpu.VMEM((2, BATCH, CHUNK), bf16),
            pltpu.VMEM((2, 2, OWN // 2, CHUNK), bf16),
            pltpu.VMEM((2, 2, OWN, CHUNK), bf16),
            pltpu.VMEM((OWN, CHUNK), f32),
            pltpu.VMEM((3, OWN, CHUNK), bf16),
            pltpu.VMEM((3, OWN, CHUNK), bf16),
            dma((9,)), dma((count,)), dma((count,)),
            dma((2, 4)), dma((2, 4)), dma((2, 4)), dma((2, 4)), dma((2, 4)), dma((2, 4)),
            dma((3,)), dma((3,)),
        ],
        compiler_params=pltpu.CompilerParams(
            collective_id=0, has_side_effects=True, vmem_limit_bytes=67043328
        ),
    )(tokens, info, gate_weight, up_weight, down_weight)


def solution(mesh):
    in_specs = (
        P("expert", None),
        P("expert", None),
        P("expert", None),
        P("expert", "tensor", None),
        P("expert", "tensor", None),
        P("expert", "tensor", None),
    )
    out_specs = P("expert", "tensor")
    return jax.shard_map(local, mesh=mesh, in_specs=in_specs, out_specs=out_specs, check_vma=False)
```

```python
import jax
import jax.numpy as jnp
from jax import lax
from jax.experimental import pallas as pl
from jax.experimental.pallas import tpu as pltpu
from jax.sharding import PartitionSpec as P

MESH = pl.DeviceIdType.MESH
f32 = jnp.float32
bf16 = jnp.bfloat16

RING = 4
OWN = 128
WIDTH = 4096
FFS = 192
HELD = 4
QUART = 1024
INFO = 16
CHUNK = 512
HID = HELD * FFS
TILE = 256
LANES = 256
BATCH = RING * OWN
ORDER = (2, 1, 3, 0)
NT = (((1,), (1,)), ((), ()))


def distance(kind, dz, dx):
    if kind == 0:
        return dx if dz == 0 else dz
    return dz if dx == 0 else dx


def transfer_ids():
    ids = {}
    for kind in range(2):
        for dz in range(RING):
            for dx in range(RING):
                if dz == 0 and dx == 0:
                    continue
                parts = ("h0", "h1") if distance(kind, dz, dx) == 2 else ("f",)
                for part in parts:
                    ids[kind, dz, dx, part] = len(ids)
                ids[kind, dz, dx, "d"] = len(ids)
    return ids


IDS = transfer_ids()


def scoped(name):
    def wrap(body):
        def inner(*args):
            with jax.named_scope(name):
                return body(*args)

        return inner

    return wrap


def kernel(
    tokens, info, wg_in, wu_in, wd_in, out,
    xa, xb, wg, wu, wd, hid, gx, mine, theirs, dgot,
    y1a, y1b, y2a, y2b, tota, totb, xsa, xsb, xg1, xg2, wrow, ys, kept, leave_y, leave_x, zy, zx,
    lsem, ssem, rsem, d_s, d_r, q_s, q_r,
):
    me = lax.axis_index("expert")
    rank = lax.axis_index("tensor")
    z, x = me // RING, me % RING
    y, c = rank // 2, rank % 2
    other = 1 - c

    def device(dz, dx, dy, core):
        return (((z + dz) % RING) * RING + (x + dx) % RING, ((y + dy) % RING) * 2 + core)

    peers = [device(0, 0, 0, other)]
    for step in (1, 3, 2):
        peers += [device(0, step, 0, c), device(step, 0, 0, c), device(0, 0, step, c)]
    barrier = pltpu.get_barrier_semaphore()
    for peer in peers:
        pl.semaphore_signal(barrier, inc=1, device_id=peer, device_id_type=MESH)

    bufs = (xa, xb)
    loads = []

    def load(src, dst):
        copy = pltpu.make_async_copy(src, dst, lsem.at[len(loads)])
        loads.append(copy)
        copy.start()
        return copy

    own_loads = []
    for half in range(2):
        own_loads.append(load(tokens.at[:, pl.ds(half * 2048, QUART)], xa.at[half, me, pl.ds(0, OWN)]))
        own_loads.append(load(info, xa.at[half, me, pl.ds(OWN, INFO)]))
        own_loads.append(load(tokens.at[:, pl.ds(half * 2048 + QUART, QUART)], xb.at[half, me]))
    weight_loads = [load(wg_in, wg), load(wu_in, wu), load(wd_in, wd)]

    def view(kind, half, dz, dx, part):
        owner = ((z + dz) % RING) * RING + (x + dx) % RING
        buf = bufs[kind]
        if part == "h0":
            return buf.at[half, owner, pl.ds(0, 64)]
        if part == "h1":
            return buf.at[half, owner, pl.ds(64, buf.shape[2] - 64)]
        return buf.at[half, owner]

    started = {}

    def describe(kind, dz, dx, part, tz, tx):
        ident = IDS[kind, (dz - tz) % RING, (dx - tx) % RING, part]
        ref = view(kind, c, dz, dx, part)
        return pltpu.make_async_remote_copy(
            src_ref=ref, dst_ref=ref, send_sem=ssem.at[ident], recv_sem=rsem.at[ident],
            device_id=device(tz, tx, 0, c), device_id_type=MESH,
        )

    def send(kind, dz, dx, part, tz, tx):
        started[describe, (kind, dz, dx, part, tz, tx)] = True
        describe(kind, dz, dx, part, tz, tx).start()

    def describe_pair(kind, dz, dx, half=c):
        ident = IDS[kind, dz, dx, "d"]
        ref = view(kind, half, dz, dx, "f")
        return pltpu.make_async_remote_copy(
            src_ref=ref, dst_ref=ref, send_sem=ssem.at[ident], recv_sem=rsem.at[ident],
            device_id=device(0, 0, 0, other), device_id_type=MESH,
        )

    def pair(kind, dz, dx):
        started[describe_pair, (kind, dz, dx)] = True
        describe_pair(kind, dz, dx).start()

    def got_pair(kind, dz, dx):
        describe_pair(kind, dz, dx, other).wait_recv()

    def got(kind, dz, dx, part):
        ident = IDS[kind, dz, dx, part]
        ref = view(kind, c, dz, dx, part)
        pltpu.make_async_remote_copy(
            src_ref=ref, dst_ref=ref, send_sem=ssem.at[ident], recv_sem=rsem.at[ident],
            device_id=device(0, 0, 0, other), device_id_type=MESH,
        ).wait_recv()

    def along(kind, first, step):
        if (kind == 0) == first:
            return (0, step)
        return (step, 0)

    def arrive(kind, first, dz, dx):
        d = distance(kind, dz, dx)
        if d == 2:
            got(kind, dz, dx, "h0")
            got(kind, dz, dx, "h1")
        else:
            got(kind, dz, dx, "f")
            if d == 3:
                send(kind, dz, dx, "h0", *along(kind, first, 1))
            else:
                send(kind, dz, dx, "h1", *along(kind, first, 3))
        pair(kind, dz, dx)

    def spread(kind, first, dz, dx):
        for step in (1, 3):
            send(kind, dz, dx, "f", *along(kind, first, step))

    def pairs(dz):
        for dx in range(RING):
            if dz or dx:
                got_pair(0, dz, dx)
                got_pair(1, dz, dx)

    queue_ids = {}

    def queued(key, src, dst, to):
        ident = queue_ids.setdefault(key, len(queue_ids))
        return pltpu.make_async_remote_copy(
            src_ref=src, dst_ref=dst, send_sem=q_s.at[ident], recv_sem=q_r.at[ident],
            device_id=to, device_id_type=MESH,
        )

    def begin(copies):
        for copy in copies:
            copy.start()

    def finish(copies):
        for copy in copies:
            copy.wait()

    def batch_z(b):
        return (b * (b + 1) // 2) % RING

    def wide(b):
        return CHUNK if b == 0 else LANES

    def y1(b):
        return y1a if b == 0 else y1b.at[b - 1]

    def y2(b):
        return y2a if b == 0 else y2b.at[b - 1]

    def tot(b):
        return tota if b == 0 else totb.at[b - 1]

    def xs(b):
        return xsa if b == 0 else xsb.at[b - 1]

    def owner_rows(dx, start, size):
        return pl.ds(pl.multiple_of(((x + dx) % RING) * OWN + start, 64), size)

    def y_copies(b, stage):
        lanes = pl.ds(0, wide(b))
        if stage == 0:
            pieces = [(mine.at[b % 3, 0, pl.ds(n * 256, 256), lanes], y1(b).at[n]) for n in range(2)]
        else:
            pieces = [(mine.at[b % 3, 1 + n, :, lanes], y2(b).at[n]) for n in range(2)]
        return [
            queued(("y", b, stage, n), src, dst, device(0, 0, (1, 3)[n], c)) for n, (src, dst) in enumerate(pieces)
        ]

    def y_last(b):
        return [
            queued(("ylast", b, d), tot(b).at[owner_rows(d, 0, OWN)], xs(b).at[d - 1], device(0, d, 0, c))
            for d in (2, 1, 3)
        ]

    @scoped("y_first")
    def y_first(b):
        begin(y_copies(b, 0))

    @scoped("y_second")
    def y_second(b):
        finish(y_copies(b, 0))
        lanes = pl.ds(0, wide(b))
        for n in range(2):
            rows = pl.ds(n * 256, 256)
            mine[b % 3, 1 + n, rows, lanes] = (
                mine[b % 3, 1 + n, rows, lanes].astype(f32) + y1(b)[n].astype(f32)
            ).astype(bf16)
        begin(y_copies(b, 1))

    @scoped("y_third")
    def y_third(b):
        finish(y_copies(b, 1))
        tot(b)[...] = (
            mine[b % 3, 3, :, pl.ds(0, wide(b))].astype(f32) + y2(b)[0].astype(f32) + y2(b)[1].astype(f32)
        ).astype(bf16)
        begin(y_last(b))

    def z_copy(b, part):
        src, dst = ((leave_y, zy), (leave_x, zx))[part]
        return queued(("z", b, part), src.at[b - 1], dst.at[b - 1], device(batch_z(b), 0, 0, c))

    @scoped("y_final")
    def y_final(b):
        finish(y_last(b))
        value = tot(b)[owner_rows(0, 0, OWN)].astype(f32)
        for n in range(3):
            value = value + xs(b)[n].astype(f32)
        if b == 0:
            kept[...] = value
        else:
            leave_y[b - 1] = value.astype(bf16)
            z_copy(b, 0).start()

    upper = pl.ds(LANES, LANES)

    def x_copies(b, stage):
        if stage == 0:
            pieces = [(mine.at[b % 3, :, owner_rows(2, 64 * n, 64), upper], xg1.at[b - 1, n]) for n in range(2)]
        else:
            pieces = [(mine.at[b % 3, :, owner_rows((1, 3)[n], 0, OWN), upper], xg2.at[b - 1, n]) for n in range(2)]
        return [
            queued(("x", b, stage, n), src, dst, device(0, (1, 3)[n], 0, c)) for n, (src, dst) in enumerate(pieces)
        ]

    def x_last(b):
        return [
            queued(("xlast", b, i), wrow.at[b - 1, i], ys.at[b - 1, i], device(0, 0, ORDER[i], c)) for i in range(3)
        ]

    @scoped("x_first")
    def x_first(b):
        begin(x_copies(b, 0))

    @scoped("x_second")
    def x_second(b):
        finish(x_copies(b, 0))
        for n in range(2):
            rows = owner_rows((1, 3)[n], 64 * n, 64)
            for i in range(4):
                mine[b % 3, i, rows, upper] = (
                    mine[b % 3, i, rows, upper].astype(f32) + xg1[b - 1, n, i].astype(f32)
                ).astype(bf16)
        begin(x_copies(b, 1))

    @scoped("x_third")
    def x_third(b):
        finish(x_copies(b, 1))
        rows = owner_rows(0, 0, OWN)
        for i in range(4):
            wrow[b - 1, i] = (
                mine[b % 3, i, rows, upper].astype(f32) + xg2[b - 1, 0, i].astype(f32) + xg2[b - 1, 1, i].astype(f32)
            ).astype(bf16)
        begin(x_last(b))

    @scoped("x_final")
    def x_final(b):
        finish(x_last(b))
        value = wrow[b - 1, 3].astype(f32)
        for i in range(3):
            value = value + ys[b - 1, i].astype(f32)
        leave_x[b - 1] = value.astype(bf16)
        z_copy(b, 1).start()

    @scoped("gates")
    def gates(zz):
        member = lax.broadcasted_iota(jnp.int32, (8, HID), 0)
        unit = lax.broadcasted_iota(jnp.int32, (8, HID), 1)
        expand = jnp.where((unit >= member * FFS) & (unit < member * FFS + FFS), 1.0, 0.0).astype(bf16)
        for o in range(RING):
            facts = xa[0, zz * RING + o, pl.ds(OWN, INFO), pl.ds(0, OWN)].astype(f32)
            named, values = facts[0:8], facts[8:16]
            found = [
                jnp.sum(jnp.where(named == (me * HELD + j).astype(f32), values, 0.0), axis=0, keepdims=True)
                for j in range(HELD)
            ]
            held = jnp.concatenate(found + [jnp.zeros((8 - HELD, OWN), f32)], axis=0).astype(bf16)
            gx[pl.ds(o * OWN, OWN)] = lax.dot_general(
                held, expand, (((0,), (0,)), ((), ())), preferred_element_type=f32
            ).astype(bf16)

    @scoped("hidden")
    def hidden(zz, i):
        units = pl.ds(i * TILE, TILE)
        gate = jnp.zeros((BATCH, TILE), f32)
        up = jnp.zeros((BATCH, TILE), f32)
        for half in range(2):
            for kind in range(2):
                block = bufs[kind][half, pl.ds(zz * RING, RING), pl.ds(0, OWN)].reshape(BATCH, QUART)
                columns = pl.ds(half * 2048 + kind * QUART, QUART)
                gate = gate + lax.dot_general(block, wg[units, columns], NT, preferred_element_type=f32)
                up = up + lax.dot_general(block, wu[units, columns], NT, preferred_element_type=f32)
        scale = gx[:, units].astype(f32)
        hid[:, units] = (gate * (1.0 / (1.0 + jnp.exp(-gate))) * up * scale).astype(bf16)

    def d_copy(s, i):
        return pltpu.make_async_remote_copy(
            src_ref=theirs.at[s, i], dst_ref=dgot.at[s, i], send_sem=d_s.at[s, i], recv_sem=d_r.at[s, i],
            device_id=device(0, 0, 0, other), device_id_type=MESH,
        )

    def down(i, core):
        column = pl.multiple_of((((y + ORDER[i]) % RING) * 2 + core) * CHUNK, CHUNK)
        return jnp.dot(hid[...], wd[:, pl.ds(column, CHUNK)], preferred_element_type=f32).astype(bf16)

    def backs(b, hook):
        s = b % 2

        def ours(i):
            with jax.named_scope("ours"):
                mine[b % 3, i] = down(i, c)

        def yours(i):
            with jax.named_scope("yours"):
                theirs[s, i] = down(i, other)
                d_copy(s, i).start()

        def join(i):
            with jax.named_scope("join"):
                d_copy(s, i).wait()
            mine[b % 3, i] = (mine[b % 3, i].astype(f32) + dgot[s, i].astype(f32)).astype(bf16)

        yours(0)
        yours(1)
        ours(0)
        yours(2)
        join(0)
        hook(4)
        yours(3)
        ours(1)
        join(1)
        hook(5)
        ours(2)
        join(2)
        hook(6)
        ours(3)
        join(3)
        hook(7)

    with jax.named_scope("enter"):
        pl.semaphore_wait(barrier, len(peers))
    with jax.named_scope("own"):
        finish(own_loads)
    spread(0, True, 0, 0)
    spread(1, True, 0, 0)
    spread(1, False, 0, 0)
    spread(0, False, 0, 0)

    with jax.named_scope("first"):
        arrive(0, True, 0, 3)
        arrive(0, True, 0, 1)
        arrive(1, True, 3, 0)
        arrive(1, True, 1, 0)
    with jax.named_scope("second"):
        arrive(1, False, 0, 3)
        arrive(1, False, 0, 1)
        spread(1, False, 1, 0)
        spread(1, False, 3, 0)
        spread(0, False, 0, 3)
        spread(0, False, 0, 1)
        arrive(0, True, 0, 2)
        spread(0, False, 0, 2)
    with jax.named_scope("opposite"):
        arrive(1, False, 0, 2)
        pairs(0)
    finish(weight_loads)

    def a(dz, dx):
        return lambda: arrive(0, False, dz, dx)

    def bb(dz, dx):
        return lambda: arrive(1, dx == 0, dz, dx)

    def run(f, *args):
        return lambda: f(*args)

    plan = {
        (0, 0): [a(1, 0), a(3, 0)],
        (0, 1): [a(3, 3), a(1, 3)],
        (0, 2): [bb(1, 3), bb(1, 1)],
        (0, 3): [a(3, 1), a(1, 1)],
        (0, 4): [run(y_first, 0)],
        (0, 5): [bb(2, 0)],
        (0, 7): [bb(3, 3), bb(3, 1), run(spread, 1, False, 2, 0)],
        (1, 0): [a(1, 2), a(3, 2), bb(1, 2), run(pairs, 1), run(y_second, 0)],
        (1, 1): [bb(3, 2)],
        (1, 3): [bb(2, 3), bb(2, 1)],
        (1, 4): [run(y_first, 1)],
        (1, 7): [run(x_first, 1)],
        (2, 0): [run(pairs, 3)],
        (2, 1): [a(2, 0), a(2, 3), a(2, 1), a(2, 2), bb(2, 2)],
        (2, 2): [run(y_third, 0), run(x_second, 1)],
        (2, 3): [run(y_second, 1)],
        (2, 4): [run(y_first, 2)],
        (2, 7): [run(x_first, 2), run(y_final, 0)],
        (3, 0): [run(pairs, 2)],
        (3, 1): [run(x_third, 1), run(y_third, 1)],
        (3, 2): [run(x_second, 2), run(y_second, 2)],
        (3, 3): [run(x_final, 1), run(y_final, 1)],
        (3, 4): [run(y_first, 3)],
        (3, 7): [run(x_first, 3), run(x_third, 2), run(y_third, 2)],
    }

    def batch(b, carry):
        def hook(point):
            for value in range(RING):
                work = plan.get((value, point), [])
                if work:

                    @pl.when(b == value)
                    def _():
                        with jax.named_scope("hook%d" % point):
                            for item in work:
                                item()

        zz = (z + batch_z(b)) % RING
        hook(0)
        gates(zz)
        for i in range(HID // TILE):
            hidden(zz, i)
            hook(1 + i)
        backs(b, hook)
        return carry

    lax.fori_loop(0, RING, batch, 0)
    y_second(3)
    x_second(3)
    y_final(2)
    x_final(2)
    y_third(3)
    x_third(3)
    y_final(3)
    x_final(3)
    with jax.named_scope("last"):
        sums = []
        for part, ref in enumerate((zy, zx)):
            total = kept[:, pl.ds(part * LANES, LANES)]
            for b in range(1, RING):
                z_copy(b, part).wait()
                total = total + ref[b - 1].astype(f32)
            out[:, pl.ds(part * LANES, LANES)] = total.astype(bf16)
    with jax.named_scope("leave"):
        for describe_one, args in started:
            describe_one(*args).wait_send()


def gate_of(scores):
    lifted = jnp.exp(scores)
    return (lifted / jnp.sum(lifted, axis=-1, keepdims=True)).astype(bf16)


def local(tokens, scores, expert_ids, gate_weight, up_weight, down_weight):
    info = jnp.concatenate([expert_ids.astype(bf16).T, gate_of(scores).T], axis=0)
    info = jnp.pad(info, ((0, 0), (0, QUART - OWN)))
    weights = [w.reshape(HID, WIDTH) for w in (gate_weight, up_weight, down_weight)]
    dma = pltpu.SemaphoreType.DMA
    count = len(IDS)
    scratch = [
        (2, 16, OWN + INFO, QUART), (2, 16, OWN, QUART),
        (HID, WIDTH), (HID, WIDTH), (HID, WIDTH),
        (BATCH, HID), (BATCH, HID),
        (3, 4, BATCH, CHUNK), (2, 4, BATCH, CHUNK), (2, 4, BATCH, CHUNK),
        (2, 256, CHUNK), (3, 2, 256, LANES),
        (2, BATCH, CHUNK), (3, 2, BATCH, LANES),
        (BATCH, CHUNK), (3, BATCH, LANES),
        (3, OWN, CHUNK), (3, 3, OWN, LANES),
        (3, 2, 4, 64, LANES), (3, 2, 4, OWN, LANES),
        (3, 4, OWN, LANES), (3, 3, OWN, LANES),
    ]
    return pl.pallas_call(
        kernel,
        out_shape=jax.ShapeDtypeStruct((OWN, CHUNK), bf16),
        in_specs=[pl.BlockSpec(memory_space=pl.ANY)] * 5,
        out_specs=pl.BlockSpec(memory_space=pltpu.VMEM),
        scratch_shapes=[pltpu.VMEM(shape, bf16) for shape in scratch]
        + [pltpu.VMEM((OWN, CHUNK), f32)]
        + [pltpu.VMEM((3, OWN, LANES), bf16)] * 4
        + [dma((9,)), dma((count,)), dma((count,)), dma((2, 4)), dma((2, 4)), dma((64,)), dma((64,))],
        compiler_params=pltpu.CompilerParams(
            collective_id=0, has_side_effects=True, vmem_limit_bytes=67043328
        ),
    )(tokens, info, *weights)


def solution(mesh):
    in_specs = (
        P("expert", None),
        P("expert", None),
        P("expert", None),
        P("expert", "tensor", None),
        P("expert", "tensor", None),
        P("expert", "tensor", None),
    )
    out_specs = P("expert", "tensor")
    return jax.shard_map(local, mesh=mesh, in_specs=in_specs, out_specs=out_specs, check_vma=False)
```

```python
import jax
import jax.numpy as jnp
from jax import lax
from jax.experimental import pallas as pl
from jax.experimental.pallas import tpu as pltpu
from jax.sharding import PartitionSpec as P

MESH = pl.DeviceIdType.MESH
f32 = jnp.float32
bf16 = jnp.bfloat16

RING = 4
OWN = 128
WIDTH = 4096
FFS = 192
HELD = 4
QUART = 1024
INFO = 16
CHUNK = 512
TOP = 8
HID = HELD * FFS
TILE = 256
LANES = 256
HALF = OWN // 2
STEPS = 2 * RING
BATCH = RING * HALF
ORDER = (2, 1, 3, 0)
NT = (((1,), (1,)), ((), ()))


def distance(kind, dz, dx):
    if kind == 0:
        return dx if dz == 0 else dz
    return dz if dx == 0 else dx


def transfer_ids():
    ids = {}
    for kind in range(2):
        for dz in range(RING):
            for dx in range(RING):
                if dz == 0:
                    continue
                ids[kind, dz, dx] = len(ids)
    for dz in range(RING):
        ids[dz] = len(ids)
    return ids


IDS = transfer_ids()


def scoped(name):
    def wrap(body):
        def inner(*args):
            with jax.named_scope(name):
                return body(*args)

        return inner

    return wrap


def kernel(
    tokens, scores, ids, wg_in, wu_in, wd_in, out,
    xall, facts, score_buf, ids_buf, wg, wu, wd, hid, gx, mine, chunk, dgot,
    y1a, y1b, y2a, y2b, tota, totb, xs1a, xs1b, xs2a, xs2b, xs3, xg1, xg2, wrow, ys1, ys2, ys3, kept, leave_y, leave_x, zy, zx,
    lsem, gsem, rsem, d_s, d_r, q_s, q_r,
):
    me = lax.axis_index("expert")
    rank = lax.axis_index("tensor")
    z, x = me // RING, me % RING
    y, c = rank // 2, rank % 2
    other = 1 - c

    def device(dz, dx, dy, core):
        return (((z + dz) % RING) * RING + (x + dx) % RING, ((y + dy) % RING) * 2 + core)

    peers = [device(0, 0, 0, other)]
    for step in (1, 3, 2):
        peers += [device(0, step, 0, c), device(step, 0, 0, c)]
    peers += [device(0, 0, step, c) for step in (1, 3, 2)]
    barrier = pltpu.get_barrier_semaphore()
    for peer in peers:
        pl.semaphore_signal(barrier, inc=1, device_id=peer, device_id_type=MESH)

    loads = []

    def load(src, dst):
        copy = pltpu.make_async_copy(src, dst, lsem.at[len(loads)])
        loads.append(copy)
        copy.start()
        return copy

    fact_loads = [load(scores, score_buf), load(ids, ids_buf)]
    own_loads = []
    for half in range(2):
        for kind in range(2):
            own_loads.append(
                load(tokens.at[:, pl.ds(half * 2048 + kind * QUART, QUART)], xall.at[kind, half, me])
            )

    def view(kind, half, dz, dx, part):
        owner = ((z + dz) % RING) * RING + (x + dx) % RING
        if part == "h0":
            return xall.at[kind, half, owner, pl.ds(0, 64)]
        if part == "h1":
            return xall.at[kind, half, owner, pl.ds(64, 64)]
        return xall.at[kind, half, owner]

    sent = {}

    def push(key, ref, to, ident, group=0):
        copy = pltpu.make_async_remote_copy(
            src_ref=ref, dst_ref=ref, send_sem=gsem.at[group], recv_sem=rsem.at[ident],
            device_id=to, device_id_type=MESH,
        )
        sent[key] = ref.size
        copy.start()

    def pull(ref, ident):
        pltpu.make_async_remote_copy(
            src_ref=ref, dst_ref=ref, send_sem=gsem.at[0], recv_sem=rsem.at[ident],
            device_id=device(0, 0, 0, other), device_id_type=MESH,
        ).wait_recv()

    def send(kind, dz, dx, part, tz, tx):
        ident = IDS[kind, (dz - tz) % RING, (dx - tx) % RING]
        push((kind, dz, dx, part, tz, tx), view(kind, c, dz, dx, part), device(tz, tx, 0, c), ident)

    def pair(kind, dz, dx):
        push((kind, dz, dx), view(kind, c, dz, dx, "f"), device(0, 0, 0, other), IDS[dz])

    def pairs(dz):
        count = RING if dz else RING - 1
        pull(xall.at[:, other, pl.ds(0, count)], IDS[dz])

    def along(kind, first, step):
        if (kind == 0) == first:
            return (0, step)
        return (step, 0)

    def arrive(kind, first, dz, dx):
        d = distance(kind, dz, dx)
        pull(view(kind, c, dz, dx, "f"), IDS[kind, dz, dx])
        if d != 2:
            if d == 3:
                send(kind, dz, dx, "h0", *along(kind, first, 1))
            else:
                send(kind, dz, dx, "h1", *along(kind, first, 3))
        pair(kind, dz, dx)

    def spread(kind, first, dz, dx):
        for step in (1, 3):
            send(kind, dz, dx, "f", *along(kind, first, step))

    queue_ids = {}

    def queued(key, src, dst, to):
        ident = queue_ids.setdefault(key, len(queue_ids))
        return pltpu.make_async_remote_copy(
            src_ref=src, dst_ref=dst, send_sem=q_s.at[ident], recv_sem=q_r.at[ident],
            device_id=to, device_id_type=MESH,
        )

    def begin(copies):
        for copy in copies:
            copy.start()

    def finish(copies):
        for copy in copies:
            copy.wait()

    def batch_z(b):
        return (b * (b + 1) // 2) % RING

    def wide(b):
        return CHUNK if b < 2 else LANES

    def y1(b):
        return y1a.at[b] if b < 2 else y1b.at[b - 2]

    def y2(b):
        return y2a.at[b] if b < 2 else y2b.at[b - 2]

    def tot(b):
        return tota.at[b] if b < 2 else totb.at[b - 2]

    def xs1(b):
        return xs1a.at[b] if b < 2 else xs1b.at[b - 2]

    def xs2(b):
        return xs2a.at[b] if b < 2 else xs2b.at[b - 2]

    def owner_rows(dx, start, size):
        return pl.ds(pl.multiple_of(((x + dx) % RING) * HALF + start, 32), size)

    def y_copies(b, stage):
        lanes = pl.ds(0, wide(b))
        if stage == 0:
            pieces = [(mine.at[b % 4, 0, pl.ds(n * 128, 128), lanes], y1(b).at[n]) for n in range(2)]
        else:
            pieces = [(mine.at[b % 4, 1 + n, :, lanes], y2(b).at[n]) for n in range(2)]
        return [
            queued(("y", b if b < 2 else 2 + b % 2, stage, n), src, dst, device(0, 0, (1, 3)[n], c)) for n, (src, dst) in enumerate(pieces)
        ]

    def direct(b):
        return b == STEPS - 1

    def y_last(b, stage):
        if direct(b):
            return [
                queued(("ydirect", d), tot(b).at[owner_rows(d, 0, HALF)], xs3.at[d - 1], device(0, d, 0, c))
                for d in (2, 1, 3)
            ]
        if stage == 0:
            pieces = [(tot(b).at[owner_rows(2, 32 * n, 32)], xs1(b).at[n]) for n in range(2)]
        else:
            pieces = [(tot(b).at[owner_rows((1, 3)[n], 0, HALF)], xs2(b).at[n]) for n in range(2)]
        return [
            queued(("ylast", b if b < 2 else 2 + b % 2, stage, n), src, dst, device(0, (1, 3)[n], 0, c)) for n, (src, dst) in enumerate(pieces)
        ]

    @scoped("y_first")
    def y_first(b):
        begin(y_copies(b, 0))

    @scoped("y_second")
    def y_second(b):
        finish(y_copies(b, 0))
        lanes = pl.ds(0, wide(b))
        for n in range(2):
            rows = pl.ds(n * 128, 128)
            mine[b % 4, 1 + n, rows, lanes] = (
                mine[b % 4, 1 + n, rows, lanes].astype(f32) + y1(b)[n].astype(f32)
            ).astype(bf16)
        begin(y_copies(b, 1))

    @scoped("y_third")
    def y_third(b):
        finish(y_copies(b, 1))
        tot(b)[...] = (
            mine[b % 4, 3, :, pl.ds(0, wide(b))].astype(f32) + y2(b)[0].astype(f32) + y2(b)[1].astype(f32)
        ).astype(bf16)
        begin(y_last(b, 0))

    @scoped("y_mid")
    def y_mid(b):
        finish(y_last(b, 0))
        for n in range(2):
            rows = owner_rows((1, 3)[n], 32 * n, 32)
            tot(b)[rows] = (tot(b)[rows].astype(f32) + xs1(b)[n].astype(f32)).astype(bf16)
        begin(y_last(b, 1))

    def z_copy(b, part):
        src, dst = ((leave_y, zy), (leave_x, zx))[part]
        return queued(("z", b, part), src.at[b - 2], dst.at[b - 2], device(batch_z(b // 2), 0, 0, c))

    @scoped("y_final")
    def y_final(b):
        finish(y_last(b, 1))
        value = tot(b)[owner_rows(0, 0, HALF)].astype(f32)
        for ref in [xs3.at[n] for n in range(3)] if direct(b) else [xs2(b).at[n] for n in range(2)]:
            value = value + ref[...].astype(f32)
        if b < 2:
            kept[pl.ds(b * HALF, HALF)] = value
        else:
            leave_y[b - 2] = value.astype(bf16)
            z_copy(b, 0).start()

    upper = pl.ds(LANES, LANES)

    def x_copies(b, stage, p):
        both = pl.ds(2 * p, 2)
        if stage == 0:
            pieces = [
                (mine.at[b % 4, both, owner_rows(2, 32 * n, 32), upper], xg1.at[b - 2, n, both]) for n in range(2)
            ]
        else:
            pieces = [
                (mine.at[b % 4, both, owner_rows((1, 3)[n], 0, HALF), upper], xg2.at[b - 2, n, both])
                for n in range(2)
            ]
        return [
            queued(("x", b % 2, stage, n, p), src, dst, device(0, (1, 3)[n], 0, c))
            for n, (src, dst) in enumerate(pieces)
        ]

    def x_last(b, stage):
        if direct(b):
            return [
                queued(("xdirect", i), wrow.at[b - 2, i], ys3.at[i], device(0, 0, ORDER[i], c)) for i in range(3)
            ]
        if stage == 0:
            pieces = [(wrow.at[b - 2, 0, pl.ds(32 * n, 32)], ys1.at[b - 2, n]) for n in range(2)]
        else:
            pieces = [(wrow.at[b - 2, 1 + n], ys2.at[b - 2, n]) for n in range(2)]
        return [
            queued(("xlast", b % 2, stage, n), src, dst, device(0, 0, (1, 3)[n], c)) for n, (src, dst) in enumerate(pieces)
        ]

    @scoped("x_first")
    def x_first(b, p):
        begin(x_copies(b, 0, p))

    @scoped("x_second")
    def x_second(b):
        for p in range(2):
            finish(x_copies(b, 0, p))
            for n in range(2):
                rows = owner_rows((1, 3)[n], 32 * n, 32)
                for i in (2 * p, 2 * p + 1):
                    mine[b % 4, i, rows, upper] = (
                        mine[b % 4, i, rows, upper].astype(f32) + xg1[b - 2, n, i].astype(f32)
                    ).astype(bf16)
            begin(x_copies(b, 1, p))

    @scoped("x_third")
    def x_third(b):
        rows = owner_rows(0, 0, HALF)
        for p in range(2):
            finish(x_copies(b, 1, p))
            for i in (2 * p, 2 * p + 1):
                wrow[b - 2, i] = (
                    mine[b % 4, i, rows, upper].astype(f32)
                    + xg2[b - 2, 0, i].astype(f32)
                    + xg2[b - 2, 1, i].astype(f32)
                ).astype(bf16)
            if p == direct(b):
                begin(x_last(b, 0))

    @scoped("x_mid")
    def x_mid(b):
        finish(x_last(b, 0))
        for n in range(2):
            rows = pl.ds(32 * n, 32)
            wrow[b - 2, 1 + n, rows] = (
                wrow[b - 2, 1 + n, rows].astype(f32) + ys1[b - 2, n].astype(f32)
            ).astype(bf16)
        begin(x_last(b, 1))

    @scoped("x_final")
    def x_final(b):
        finish(x_last(b, 1))
        value = wrow[b - 2, 3].astype(f32)
        for ref in [ys3.at[n] for n in range(3)] if direct(b) else [ys2.at[b - 2, n] for n in range(2)]:
            value = value + ref[...].astype(f32)
        leave_x[b - 2] = value.astype(bf16)
        z_copy(b, 1).start()

    @scoped("gates")
    def gates(zz):
        member = lax.broadcasted_iota(jnp.int32, (8, HID), 0)
        unit = lax.broadcasted_iota(jnp.int32, (8, HID), 1)
        expand = jnp.where((unit >= member * FFS) & (unit < member * FFS + FFS), 1.0, 0.0).astype(bf16)
        for o in range(RING):
            about = facts[zz * RING + o].astype(f32)
            named, values = about[0:8], about[8:16]
            found = [
                jnp.sum(jnp.where(named == (me * HELD + j).astype(f32), values, 0.0), axis=0, keepdims=True)
                for j in range(HELD)
            ]
            held = jnp.concatenate(found + [jnp.zeros((8 - HELD, OWN), f32)], axis=0).astype(bf16)
            gx[zz * RING + o] = lax.dot_general(
                held, expand, (((0,), (0,)), ((), ())), preferred_element_type=f32
            ).astype(bf16)

    @scoped("hidden")
    def hidden(zz, rows, i):
        units = pl.ds(i * TILE, TILE)
        gate = jnp.zeros((BATCH, TILE), f32)
        up = jnp.zeros((BATCH, TILE), f32)
        for half in range(2):
            for kind in range(2):
                block = xall[kind, half, pl.ds(zz * RING, RING), rows].reshape(BATCH, QUART)
                columns = pl.ds(half * 2048 + kind * QUART, QUART)
                gate = gate + lax.dot_general(block, wg[units, columns], NT, preferred_element_type=f32)
                up = up + lax.dot_general(block, wu[units, columns], NT, preferred_element_type=f32)
        scale = gx[pl.ds(zz * RING, RING), rows, units].reshape(BATCH, TILE).astype(f32)
        hid[:, units] = (gate * (1.0 / (1.0 + jnp.exp(-gate))) * up * scale).astype(bf16)

    def d_copy(s, i):
        return pltpu.make_async_remote_copy(
            src_ref=chunk.at[i, other], dst_ref=dgot.at[s, i], send_sem=d_s.at[s, i], recv_sem=d_r.at[s, i],
            device_id=device(0, 0, 0, other), device_id_type=MESH,
        )

    def down(s, i):
        with jax.named_scope("down"):
            column = pl.multiple_of(((y + ORDER[i]) % RING) * 2 * CHUNK, CHUNK)
            value = jnp.dot(hid[...], wd[:, pl.ds(column, 2 * CHUNK)], preferred_element_type=f32).astype(bf16)
            chunk[i, 0] = value[:, :CHUNK]
            chunk[i, 1] = value[:, CHUNK:]
            d_copy(s, i).start()

    def join(b, s, i):
        with jax.named_scope("join"):
            d_copy(s, i).wait()
        mine[b % 4, i] = (chunk[i, c].astype(f32) + dgot[s, i].astype(f32)).astype(bf16)

    def backs(b, hook):
        s = b % 2
        down(s, 0)
        down(s, 1)
        down(s, 2)
        join(b, s, 0)
        hook(4)
        down(s, 3)
        join(b, s, 1)
        hook(5)
        join(b, s, 2)
        hook(6)

    def fact_copies(stage):
        if stage == 0:
            for d in (2, 1, 3):
                push(("fx", d), facts.at[me], device(0, d, 0, c), len(IDS), 1)
        else:
            for d in (2, 1, 3):
                push(("fz", d), facts.at[pl.ds(z * RING, RING)], device(d, 0, 0, c), len(IDS) + 1, 1)

    def fact_waits(stage):
        pull(facts.at[pl.ds(0, 12 if stage else 3)], len(IDS) + stage)

    finish(fact_loads)
    lifted = jnp.exp(score_buf[...])
    gate_values = (lifted / jnp.sum(lifted, axis=0, keepdims=True)).astype(bf16).astype(f32)
    facts[me] = jnp.concatenate([ids_buf[...].astype(f32), gate_values], axis=0).astype(bf16)

    with jax.named_scope("enter"):
        pl.semaphore_wait(barrier, len(peers))
    with jax.named_scope("own"):
        finish(own_loads)
    parity = y % 2

    def own_view(dx, h, lanes):
        owner = z * RING + (x + dx) % RING
        rows = pl.ds(0, OWN) if h is None else pl.ds(64 * h, 64)
        return xall.at[:, c, owner, rows, pl.ds(pl.multiple_of(lanes * CHUNK, CHUNK), CHUNK)]

    own_ids = {}

    def own_send(axis, dx, h, step):
        key = ("x", (dx - step) % RING, h) if axis == "x" else ("y", dx)
        ident = own_ids.setdefault(key, len(IDS) + 2 + len(own_ids))
        to = device(0, step, 0, c) if axis == "x" else device(0, 0, step, c)
        push((axis, dx, h, step), own_view(dx, h, parity), to, ident)

    def own_got(axis, dx, h):
        if axis == "x":
            pull(own_view(dx, h, parity), own_ids["x", dx, h])
        else:
            pull(own_view(dx, None, 1 - parity), own_ids["y", dx])

    def sideways(dx, h):
        own_send("y", dx, h, (1, 3)[h])

    fact_copies(0)
    own_send("x", 0, 0, 1)
    own_send("x", 0, 1, 3)
    own_send("x", 0, 1, 1)
    own_send("x", 0, 0, 3)
    spread(1, True, 0, 0)
    fact_waits(0)
    fact_copies(1)
    spread(0, False, 0, 0)

    weight_loads = [load(wg_in, wg), load(wu_in, wu), load(wd_in, wd)]
    with jax.named_scope("ox1"):
        own_got("x", 3, 0)
        own_send("x", 3, 0, 1)
        sideways(3, 0)
        own_got("x", 1, 1)
        own_send("x", 1, 1, 3)
        sideways(1, 1)
    with jax.named_scope("ox2"):
        own_got("x", 3, 1)
        sideways(3, 1)
        own_got("x", 1, 0)
        sideways(1, 0)
    with jax.named_scope("bz"):
        arrive(1, True, 3, 0)
        arrive(1, True, 1, 0)
    with jax.named_scope("ox3"):
        own_got("x", 2, 0)
        sideways(2, 0)
        own_got("x", 2, 1)
        sideways(2, 1)
        spread(1, False, 1, 0)
        spread(1, False, 3, 0)
    gates(z)
    with jax.named_scope("fz"):
        fact_waits(1)
    gates((z + 1) % RING)
    gates((z + 2) % RING)
    for dx in (3, 1, 2):
        with jax.named_scope("oy%d" % dx):
            own_got("y", dx, 0)
            spread(0, False, 0, dx)
            pair(0, 0, dx)
            pair(1, 0, dx)
        if dx == 1:
            gates((z + 3) % RING)
    with jax.named_scope("pairs"):
        pairs(0)
    finish(weight_loads)

    def a(dz, dx):
        return lambda: arrive(0, False, dz, dx)

    def bb(dz, dx):
        return lambda: arrive(1, dx == 0, dz, dx)

    def run(f, *args):
        return lambda: f(*args)

    def xf(b, i):
        return run(x_first, b, i)

    plan = {
        (0, 0): [a(1, 0), a(3, 0)],
        (0, 1): [bb(1, 3), bb(1, 1)],
        (0, 5): [a(3, 3), a(1, 3)],
        (1, 0): [bb(3, 3), bb(3, 1), bb(2, 0), run(spread, 1, False, 2, 0)],
        (1, 2): [a(3, 1), a(1, 1)],
        (2, 0): [a(1, 2), a(3, 2), bb(1, 2), bb(3, 2), run(pairs, 1)],
        (3, 0): [bb(2, 3), bb(2, 1)],
        (4, 0): [run(pairs, 3)],
        (4, 1): [a(2, 0), a(2, 3), a(2, 1), bb(2, 2), a(2, 2)],
        (6, 0): [run(pairs, 2)],
    }

    def later(step, point, work):
        plan.setdefault((step, point), []).append(work)

    for b in range(STEPS):
        later(b, 4, run(y_first, b))
        if b > 1:
            later(b, 5, run(x_first, b, 0))
            later(b + 1, 1, run(x_first, b, 1))
    for step in range(STEPS):
        for lag, point, work in (
            (3, 1, x_mid), (3, 1, y_mid), (2, 3, y_third), (2, 3, x_third),
            (1, 3, y_second), (1, 4, x_second), (3, 6, y_final), (3, 6, x_final),
        ):
            if step - lag > 1:
                later(step, point, run(work, step - lag))
    for b in range(2):
        later(b + 1, 4, run(y_second, b))
        later(b + 3, 1, run(y_third, b))
        later(b + 4, 1, run(y_mid, b))
        later(b + 5, 1, run(y_final, b))

    def batch(b, carry):
        def hook(point):
            for value in range(STEPS):
                work = plan.get((value, point), [])
                if work:

                    @pl.when(b == value)
                    def _():
                        with jax.named_scope("hook%d" % point):
                            for item in work:
                                item()

        zz = (z + batch_z(b // 2)) % RING
        rows = pl.ds(pl.multiple_of((b % 2) * HALF, HALF), HALF)
        hook(0)
        for i in range(HID // TILE):
            hidden(zz, rows, i)
            if i == 0:

                @pl.when(b > 0)
                def _():
                    join(b + 3, (b + 1) % 2, 3)

            hook(1 + i)
        backs(b, hook)
        return carry

    lax.fori_loop(0, STEPS, batch, 0)
    join(STEPS - 1, (STEPS - 1) % 2, 3)
    final = STEPS - 1
    x_first(final, 1)
    x_mid(final - 2)
    y_mid(final - 2)
    y_second(final)
    x_second(final)
    y_third(final - 1)
    x_third(final - 1)
    y_final(final - 2)
    x_final(final - 2)
    y_mid(final - 1)
    x_mid(final - 1)
    y_third(final)
    x_third(final)
    for b in (final - 1, final):
        y_final(b)
        x_final(b)
    with jax.named_scope("last"):
        for part, ref in enumerate((zy, zx)):
            for h in range(2):
                rows, lanes = pl.ds(h * HALF, HALF), pl.ds(part * LANES, LANES)
                total = kept[rows, lanes]
                for b in range(2 + h, STEPS, 2):
                    z_copy(b, part).wait()
                    total = total + ref[b - 2].astype(f32)
                out[rows, lanes] = total.astype(bf16)
    with jax.named_scope("leave"):
        block = OWN * QUART
        small = sum(size for key, size in sent.items() if key[0] in ("fx", "fz"))
        blocks = (sum(sent.values()) - small) // block
        assert blocks * block + small == sum(sent.values())
        assert blocks == 60 and small == 15 * INFO * OWN
        for group, ref in enumerate((xall.at[:, :, pl.ds(0, 15)], facts.at[pl.ds(0, 15)])):
            pltpu.make_async_remote_copy(
                src_ref=ref, dst_ref=ref, send_sem=gsem.at[group], recv_sem=rsem.at[0],
                device_id=device(0, 0, 0, other), device_id_type=MESH,
            ).wait_send()


def local(tokens, scores, expert_ids, gate_weight, up_weight, down_weight):
    weights = [w.reshape(HID, WIDTH) for w in (gate_weight, up_weight, down_weight)]
    dma = pltpu.SemaphoreType.DMA
    count = len(IDS)
    scratch = [
        (HID, WIDTH), (HID, WIDTH), (HID, WIDTH),
        (BATCH, HID), (RING * RING, OWN, HID),
        (4, 4, BATCH, CHUNK), (4, 2, BATCH, CHUNK), (2, 4, BATCH, CHUNK),
        (2, 2, 128, CHUNK), (6, 2, 128, LANES),
        (2, 2, BATCH, CHUNK), (6, 2, BATCH, LANES),
        (2, BATCH, CHUNK), (6, BATCH, LANES),
        (2, 2, 32, CHUNK), (6, 2, 32, LANES), (2, 2, HALF, CHUNK), (6, 2, HALF, LANES), (3, HALF, LANES),
        (6, 2, 4, 32, LANES), (6, 2, 4, HALF, LANES),
        (6, 4, HALF, LANES), (6, 2, 32, LANES), (6, 2, HALF, LANES), (3, HALF, LANES),
    ]
    return pl.pallas_call(
        kernel,
        out_shape=jax.ShapeDtypeStruct((OWN, CHUNK), bf16),
        in_specs=[pl.BlockSpec(memory_space=pl.ANY)] * 6,
        out_specs=pl.BlockSpec(memory_space=pltpu.VMEM),
        scratch_shapes=[
            pltpu.VMEM((2, 2, 16, OWN, QUART), bf16), pltpu.VMEM((16, INFO, OWN), bf16),
            pltpu.VMEM((TOP, OWN), f32), pltpu.VMEM((TOP, OWN), jnp.int32),
        ]
        + [pltpu.VMEM(shape, bf16) for shape in scratch]
        + [pltpu.VMEM((OWN, CHUNK), f32)]
        + [pltpu.VMEM((6, HALF, LANES), bf16)] * 4
        + [dma((9,)), dma((2,)), dma((count + 11,)), dma((2, 4)), dma((2, 4)), dma((74,)), dma((74,))],
        compiler_params=pltpu.CompilerParams(
            collective_id=0, has_side_effects=True, vmem_limit_bytes=67043328
        ),
    )(tokens, scores.T, expert_ids.T, *weights)


def solution(mesh):
    in_specs = (
        P("expert", None),
        P("expert", None),
        P("expert", None),
        P("expert", "tensor", None),
        P("expert", "tensor", None),
        P("expert", "tensor", None),
    )
    out_specs = P("expert", "tensor")
    return jax.shard_map(local, mesh=mesh, in_specs=in_specs, out_specs=out_specs, check_vma=False)
```

```python
import jax
import jax.numpy as jnp
from jax import lax
from jax.experimental import pallas as pl
from jax.experimental.pallas import tpu as pltpu
from jax.sharding import PartitionSpec as P

MESH = pl.DeviceIdType.MESH
f32 = jnp.float32
bf16 = jnp.bfloat16

RING = 4
OWN = 128
WIDTH = 4096
FFS = 192
HELD = 4
QUART = 1024
FIRST = 768
INFO = 16
CHUNK = 512
TOP = 8
HID = HELD * FFS
TILE = 256
LANES = 256
HALF = OWN // 2
STEPS = 2 * RING
BATCH = RING * HALF
ORDER = (2, 1, 3, 0)
NT = (((1,), (1,)), ((), ()))


def distance(kind, dz, dx):
    if kind == 0:
        return dx if dz == 0 else dz
    return dz if dx == 0 else dx


def transfer_ids():
    ids = {}
    for kind in range(2):
        for dz in range(RING):
            for dx in range(RING):
                if dz == 0:
                    continue
                ids[kind, dz, dx] = len(ids)
    for dz in range(RING):
        ids[dz] = len(ids)
    return ids


IDS = transfer_ids()


def scoped(name):
    def wrap(body):
        def inner(*args):
            with jax.named_scope(name):
                return body(*args)

        return inner

    return wrap


def kernel(
    tokens, scores, ids, wg_in, wu_in, wd_in, out,
    xall, facts, score_buf, ids_buf, wg, wu, wd, hid, gx, mine, chunk, dgot,
    y1a, y1b, y2a, y2b, tota, totb, xs1a, xs1b, xs2a, xs2b, xs3, xg1, xg2, wrow, ys1, ys2, ys3, kept, leave_y, leave_x, zy, zx,
    lsem, gsem, rsem, d_s, d_r, q_s, q_r,
):
    me = lax.axis_index("expert")
    rank = lax.axis_index("tensor")
    z, x = me // RING, me % RING
    y, c = rank // 2, rank % 2
    other = 1 - c

    def device(dz, dx, dy, core):
        return (((z + dz) % RING) * RING + (x + dx) % RING, ((y + dy) % RING) * 2 + core)

    peers = [device(0, 0, 0, other)]
    for step in (1, 3, 2):
        peers += [device(0, step, 0, c), device(step, 0, 0, c)]
    peers += [device(0, 0, step, c) for step in (1, 3, 2)]
    barrier = pltpu.get_barrier_semaphore()
    for peer in peers:
        pl.semaphore_signal(barrier, inc=1, device_id=peer, device_id_type=MESH)

    loads = []

    def load(src, dst):
        copy = pltpu.make_async_copy(src, dst, lsem.at[len(loads)])
        loads.append(copy)
        copy.start()
        return copy

    fact_loads = [load(scores, score_buf), load(ids, ids_buf)]
    own_loads = []
    for half in range(2):
        own_loads.append(load(tokens.at[:, pl.ds(half * 2 * QUART, 2 * QUART)], xall.at[half, me]))

    def view(kind, half, dz, dx, part):
        owner = ((z + dz) % RING) * RING + (x + dx) % RING
        rows = {"h0": pl.ds(0, 64), "h1": pl.ds(64, 64), "f": pl.ds(0, OWN)}[part]
        lanes = pl.ds(FIRST, 2 * QUART - FIRST) if kind else pl.ds(0, FIRST)
        return xall.at[half, owner, rows, lanes]

    sent = {}

    def push(key, ref, to, ident, group=0):
        copy = pltpu.make_async_remote_copy(
            src_ref=ref, dst_ref=ref, send_sem=gsem.at[group], recv_sem=rsem.at[ident],
            device_id=to, device_id_type=MESH,
        )
        sent[key] = ref.size
        copy.start()

    def pull(ref, ident):
        pltpu.make_async_remote_copy(
            src_ref=ref, dst_ref=ref, send_sem=gsem.at[0], recv_sem=rsem.at[ident],
            device_id=device(0, 0, 0, other), device_id_type=MESH,
        ).wait_recv()

    def send(kind, dz, dx, part, tz, tx):
        ident = IDS[kind, (dz - tz) % RING, (dx - tx) % RING]
        push((kind, dz, dx, part, tz, tx), view(kind, c, dz, dx, part), device(tz, tx, 0, c), ident)

    def pair(kind, dz, dx):
        push((kind, dz, dx), view(kind, c, dz, dx, "f"), device(0, 0, 0, other), IDS[dz])

    def pairs(dz):
        count = RING if dz else RING - 1
        pull(xall.at[other, pl.ds(0, count)], IDS[dz])

    def along(kind, first, step):
        if (kind == 0) == first:
            return (0, step)
        return (step, 0)

    def arrive(kind, first, dz, dx):
        d = distance(kind, dz, dx)
        pull(view(kind, c, dz, dx, "f"), IDS[kind, dz, dx])
        if d != 2:
            if d == 3:
                send(kind, dz, dx, "h0", *along(kind, first, 1))
            else:
                send(kind, dz, dx, "h1", *along(kind, first, 3))
        pair(kind, dz, dx)

    def spread(kind, first, dz, dx):
        for step in (1, 3):
            send(kind, dz, dx, "f", *along(kind, first, step))

    queue_ids = {}

    def queued(key, src, dst, to):
        ident = queue_ids.setdefault(key, len(queue_ids))
        return pltpu.make_async_remote_copy(
            src_ref=src, dst_ref=dst, send_sem=q_s.at[ident], recv_sem=q_r.at[ident],
            device_id=to, device_id_type=MESH,
        )

    def begin(copies):
        for copy in copies:
            copy.start()

    def finish(copies):
        for copy in copies:
            copy.wait()

    def batch_z(b):
        return (b * (b + 1) // 2) % RING

    def wide(b):
        return CHUNK if b < 2 else LANES

    def y1(b):
        return y1a.at[b] if b < 2 else y1b.at[b - 2]

    def y2(b):
        return y2a.at[b] if b < 2 else y2b.at[b - 2]

    def tot(b):
        return tota.at[b] if b < 2 else totb.at[b - 2]

    def xs1(b):
        return xs1a.at[b] if b < 2 else xs1b.at[b - 2]

    def xs2(b):
        return xs2a.at[b] if b < 2 else xs2b.at[b - 2]

    def owner_rows(dx, start, size):
        return pl.ds(pl.multiple_of(((x + dx) % RING) * HALF + start, 32), size)

    def y_copies(b, stage):
        lanes = pl.ds(0, wide(b))
        if stage == 0:
            pieces = [(mine.at[b % 4, 0, pl.ds(n * 128, 128), lanes], y1(b).at[n]) for n in range(2)]
        else:
            pieces = [(mine.at[b % 4, 1 + n, :, lanes], y2(b).at[n]) for n in range(2)]
        return [
            queued(("y", b if b < 2 else 2 + b % 2, stage, n), src, dst, device(0, 0, (1, 3)[n], c)) for n, (src, dst) in enumerate(pieces)
        ]

    def direct(b):
        return b >= STEPS - 3

    def y_last(b, stage):
        if direct(b):
            return [
                queued(("ydirect", b, d), tot(b).at[owner_rows(d, 0, HALF)], xs3.at[b - STEPS + 3, d - 1], device(0, d, 0, c))
                for d in (2, 1, 3)
            ]
        if stage == 0:
            pieces = [(tot(b).at[owner_rows(2, 32 * n, 32)], xs1(b).at[n]) for n in range(2)]
        else:
            pieces = [(tot(b).at[owner_rows((1, 3)[n], 0, HALF)], xs2(b).at[n]) for n in range(2)]
        return [
            queued(("ylast", b if b < 2 else 2 + b % 2, stage, n), src, dst, device(0, (1, 3)[n], 0, c)) for n, (src, dst) in enumerate(pieces)
        ]

    @scoped("y_first")
    def y_first(b):
        begin(y_copies(b, 0))

    @scoped("y_second")
    def y_second(b):
        finish(y_copies(b, 0))
        lanes = pl.ds(0, wide(b))
        for n in range(2):
            rows = pl.ds(n * 128, 128)
            mine[b % 4, 1 + n, rows, lanes] = (
                mine[b % 4, 1 + n, rows, lanes].astype(f32) + y1(b)[n].astype(f32)
            ).astype(bf16)
        begin(y_copies(b, 1))

    @scoped("y_third")
    def y_third(b):
        finish(y_copies(b, 1))
        tot(b)[...] = (
            mine[b % 4, 3, :, pl.ds(0, wide(b))].astype(f32) + y2(b)[0].astype(f32) + y2(b)[1].astype(f32)
        ).astype(bf16)
        begin(y_last(b, 0))

    @scoped("y_mid")
    def y_mid(b):
        finish(y_last(b, 0))
        for n in range(2):
            rows = owner_rows((1, 3)[n], 32 * n, 32)
            tot(b)[rows] = (tot(b)[rows].astype(f32) + xs1(b)[n].astype(f32)).astype(bf16)
        begin(y_last(b, 1))

    def z_copy(b, part):
        src, dst = ((leave_y, zy), (leave_x, zx))[part]
        return queued(("z", b, part), src.at[b - 2], dst.at[b - 2], device(batch_z(b // 2), 0, 0, c))

    @scoped("y_final")
    def y_final(b):
        finish(y_last(b, 1))
        value = tot(b)[owner_rows(0, 0, HALF)].astype(f32)
        for ref in [xs3.at[b - STEPS + 3, n] for n in range(3)] if direct(b) else [xs2(b).at[n] for n in range(2)]:
            value = value + ref[...].astype(f32)
        if b < 2:
            kept[pl.ds(b * HALF, HALF)] = value
        else:
            leave_y[b - 2] = value.astype(bf16)
            z_copy(b, 0).start()

    upper = pl.ds(LANES, LANES)

    def x_copies(b, stage, p):
        both = pl.ds(2 * p, 2)
        if stage == 0:
            pieces = [
                (mine.at[b % 4, both, owner_rows(2, 32 * n, 32), upper], xg1.at[b - 2, n, both]) for n in range(2)
            ]
        else:
            pieces = [
                (mine.at[b % 4, both, owner_rows((1, 3)[n], 0, HALF), upper], xg2.at[b - 2, n, both])
                for n in range(2)
            ]
        return [
            queued(("x", b % 2 + b // (STEPS - 1), stage, n, p), src, dst, device(0, (1, 3)[n], 0, c))
            for n, (src, dst) in enumerate(pieces)
        ]

    def x_last(b, stage):
        if direct(b):
            return [
                queued(("xdirect", b, i), wrow.at[b - 2, i], ys3.at[b - STEPS + 3, i], device(0, 0, ORDER[i], c)) for i in range(3)
            ]
        if stage == 0:
            pieces = [(wrow.at[b - 2, 0, pl.ds(32 * n, 32)], ys1.at[b - 2, n]) for n in range(2)]
        else:
            pieces = [(wrow.at[b - 2, 1 + n], ys2.at[b - 2, n]) for n in range(2)]
        return [
            queued(("xlast", b % 2, stage, n), src, dst, device(0, 0, (1, 3)[n], c)) for n, (src, dst) in enumerate(pieces)
        ]

    @scoped("x_first")
    def x_first(b, p):
        begin(x_copies(b, 0, p))

    @scoped("x_second")
    def x_second(b):
        for p in range(2):
            finish(x_copies(b, 0, p))
            for n in range(2):
                rows = owner_rows((1, 3)[n], 32 * n, 32)
                for i in (2 * p, 2 * p + 1):
                    mine[b % 4, i, rows, upper] = (
                        mine[b % 4, i, rows, upper].astype(f32) + xg1[b - 2, n, i].astype(f32)
                    ).astype(bf16)
            begin(x_copies(b, 1, p))

    @scoped("x_third")
    def x_third(b):
        rows = owner_rows(0, 0, HALF)
        for p in range(2):
            finish(x_copies(b, 1, p))
            for i in (2 * p, 2 * p + 1):
                wrow[b - 2, i] = (
                    mine[b % 4, i, rows, upper].astype(f32)
                    + xg2[b - 2, 0, i].astype(f32)
                    + xg2[b - 2, 1, i].astype(f32)
                ).astype(bf16)
            if p == direct(b):
                begin(x_last(b, 0))

    @scoped("x_mid")
    def x_mid(b):
        finish(x_last(b, 0))
        for n in range(2):
            rows = pl.ds(32 * n, 32)
            wrow[b - 2, 1 + n, rows] = (
                wrow[b - 2, 1 + n, rows].astype(f32) + ys1[b - 2, n].astype(f32)
            ).astype(bf16)
        begin(x_last(b, 1))

    @scoped("x_final")
    def x_final(b):
        finish(x_last(b, 1))
        value = wrow[b - 2, 3].astype(f32)
        for ref in [ys3.at[b - STEPS + 3, n] for n in range(3)] if direct(b) else [ys2.at[b - 2, n] for n in range(2)]:
            value = value + ref[...].astype(f32)
        leave_x[b - 2] = value.astype(bf16)
        z_copy(b, 1).start()

    @scoped("gates")
    def gates(zz):
        member = lax.broadcasted_iota(jnp.int32, (8, HID), 0)
        unit = lax.broadcasted_iota(jnp.int32, (8, HID), 1)
        expand = jnp.where((unit >= member * FFS) & (unit < member * FFS + FFS), 1.0, 0.0).astype(bf16)
        for o in range(RING):
            about = facts[zz * RING + o].astype(f32)
            named, values = about[0:8], about[8:16]
            found = [
                jnp.sum(jnp.where(named == (me * HELD + j).astype(f32), values, 0.0), axis=0, keepdims=True)
                for j in range(HELD)
            ]
            held = jnp.concatenate(found + [jnp.zeros((8 - HELD, OWN), f32)], axis=0).astype(bf16)
            gx[zz * RING + o] = lax.dot_general(
                held, expand, (((0,), (0,)), ((), ())), preferred_element_type=f32
            ).astype(bf16)

    @scoped("hidden")
    def hidden(load_block, load_scale, count, i):
        units = pl.ds(i * TILE, TILE)
        gate = jnp.zeros((count * OWN, TILE), f32)
        up = jnp.zeros((count * OWN, TILE), f32)
        for half in range(2):
            for q in range(2):
                block = load_block(half, pl.ds(q * QUART, QUART))
                columns = pl.ds((half * 2 + q) * QUART, QUART)
                gate = gate + lax.dot_general(block, wg[units, columns], NT, preferred_element_type=f32)
                up = up + lax.dot_general(block, wu[units, columns], NT, preferred_element_type=f32)
        scale = load_scale(units).astype(f32)
        return (gate * (1.0 / (1.0 + jnp.exp(-gate))) * up * scale).astype(bf16)

    def hidden_row(zz, i):
        owners = pl.ds(zz * RING, RING)
        value = hidden(
            lambda half, lanes: xall[half, owners, :, lanes].reshape(RING * OWN, QUART),
            lambda units: gx[owners, :, units].reshape(RING * OWN, TILE),
            RING,
            i,
        )
        hid[:, :, pl.ds(i * TILE, TILE)] = value.reshape(RING, OWN, TILE)

    def hidden_owners(steps, i):
        places = [(x + d) % RING for d in steps]
        owners = [z * RING + place for place in places]
        value = hidden(
            lambda half, lanes: jnp.concatenate([xall[half, o, :, lanes] for o in owners], axis=0),
            lambda units: jnp.concatenate([gx[o, :, units] for o in owners], axis=0),
            len(owners),
            i,
        )
        for n, place in enumerate(places):
            hid[place, :, pl.ds(i * TILE, TILE)] = value[n * OWN : (n + 1) * OWN]

    def d_copy(s, i):
        return pltpu.make_async_remote_copy(
            src_ref=chunk.at[i, other], dst_ref=dgot.at[s, i], send_sem=d_s.at[s, i], recv_sem=d_r.at[s, i],
            device_id=device(0, 0, 0, other), device_id_type=MESH,
        )

    def down(rows, s, i):
        with jax.named_scope("down"):
            column = pl.multiple_of(((y + ORDER[i]) % RING) * 2 * CHUNK, CHUNK)
            value = jnp.dot(hid[:, rows, :].reshape(BATCH, HID), wd[:, pl.ds(column, 2 * CHUNK)], preferred_element_type=f32).astype(bf16)
            chunk[i, 0] = value[:, :CHUNK]
            chunk[i, 1] = value[:, CHUNK:]
            d_copy(s, i).start()

    def join(b, s, i):
        with jax.named_scope("join"):
            d_copy(s, i).wait()
        mine[b % 4, i] = (chunk[i, c].astype(f32) + dgot[s, i].astype(f32)).astype(bf16)

    def backs(b, rows, hook):
        s = b % 2
        down(rows, s, 0)

        @pl.when(s == 1)
        def _():
            join(b + 3, 0, 3)

        hook(3)
        down(rows, s, 1)
        down(rows, s, 2)
        join(b, s, 0)
        hook(4)
        down(rows, s, 3)
        join(b, s, 1)
        hook(5)
        join(b, s, 2)
        hook(6)

    def fact_copies(stage):
        if stage == 0:
            for d in (2, 1, 3):
                push(("fx", d), facts.at[me], device(0, d, 0, c), len(IDS), 1)
        else:
            for d in (2, 1, 3):
                push(("fz", d), facts.at[pl.ds(z * RING, RING)], device(d, 0, 0, c), len(IDS) + 1, 1)

    def fact_waits(stage):
        pull(facts.at[pl.ds(0, 12 if stage else 3)], len(IDS) + stage)

    finish(fact_loads)
    lifted = jnp.exp(score_buf[...])
    gate_values = (lifted / jnp.sum(lifted, axis=0, keepdims=True)).astype(bf16).astype(f32)
    facts[me] = jnp.concatenate([ids_buf[...].astype(f32), gate_values], axis=0).astype(bf16)

    with jax.named_scope("enter"):
        pl.semaphore_wait(barrier, len(peers))
    with jax.named_scope("own"):
        finish(own_loads)
    parity = y % 2

    def own_view(dx, h, lanes):
        owner = z * RING + (x + dx) % RING
        rows = pl.ds(0, OWN) if h is None else pl.ds(64 * h, 64)
        return xall.at[c, owner, rows, pl.ds(pl.multiple_of(lanes * QUART, QUART), QUART)]

    own_ids = {}

    def own_send(axis, dx, h, step):
        key = ("x", (dx - step) % RING, h) if axis == "x" else ("y", dx)
        ident = own_ids.setdefault(key, len(IDS) + 2 + len(own_ids))
        to = device(0, step, 0, c) if axis == "x" else device(0, 0, step, c)
        push((axis, dx, h, step), own_view(dx, h, parity), to, ident)

    def own_got(axis, dx, h):
        if axis == "x":
            pull(own_view(dx, h, parity), own_ids["x", dx, h])
        else:
            pull(own_view(dx, None, 1 - parity), own_ids["y", dx])

    def sideways(dx, h):
        own_send("y", dx, h, (1, 3)[h])

    fact_copies(0)
    own_send("x", 0, 0, 1)
    own_send("x", 0, 1, 3)
    own_send("x", 0, 1, 1)
    own_send("x", 0, 0, 3)
    spread(1, True, 0, 0)
    fact_waits(0)
    fact_copies(1)
    spread(0, False, 0, 0)

    weight_loads = [load(wg_in, wg), load(wu_in, wu), load(wd_in, wd)]
    with jax.named_scope("ox1"):
        own_got("x", 3, 0)
        own_send("x", 3, 0, 1)
        sideways(3, 0)
        own_got("x", 1, 1)
        own_send("x", 1, 1, 3)
        sideways(1, 1)
    finish(weight_loads[:2])
    gates(z)
    hidden_owners((0,), 0)
    with jax.named_scope("ox2"):
        own_got("x", 3, 1)
        sideways(3, 1)
        own_got("x", 1, 0)
        sideways(1, 0)
    with jax.named_scope("bz"):
        arrive(1, True, 3, 0)
        arrive(1, True, 1, 0)
    with jax.named_scope("ox3"):
        own_got("x", 2, 0)
        sideways(2, 0)
        own_got("x", 2, 1)
        sideways(2, 1)
        spread(1, False, 1, 0)
        spread(1, False, 3, 0)
    with jax.named_scope("fz"):
        fact_waits(1)
    hidden_owners((0,), 1)
    hidden_owners((0,), 2)
    for dx in (3, 1, 2):
        with jax.named_scope("oy%d" % dx):
            own_got("y", dx, 0)
            spread(0, False, 0, dx)
            pair(0, 0, dx)
            pair(1, 0, dx)
        if dx != 2:
            gates((z + dx) % RING)
    with jax.named_scope("pairs"):
        pairs(0)
    finish(weight_loads[2:])

    def a(dz, dx):
        return lambda: arrive(0, False, dz, dx)

    def bb(dz, dx):
        return lambda: arrive(1, dx == 0, dz, dx)

    def run(f, *args):
        return lambda: f(*args)

    def xf(b, i):
        return run(x_first, b, i)

    plan = {
        (0, 0): [a(1, 0), a(3, 0)],
        (0, 2): [bb(1, 3), bb(1, 1)],
        (0, 4): [a(3, 3), a(1, 3)],
        (1, 3): [a(3, 1), a(1, 1), bb(3, 3), bb(3, 1)],
        (1, 4): [bb(2, 0), run(spread, 1, False, 2, 0)],
        (2, 0): [run(gates, (z + 2) % RING), a(1, 2), a(3, 2), bb(1, 2), run(pairs, 1), run(y_second, 0)],
        (2, 1): [run(y_second, 1)],
        (2, 4): [run(y_third, 0)],
        (3, 0): [bb(3, 2)],
        (2, 6): [bb(2, 3), bb(2, 1)],
        (3, 6): [run(y_mid, 0), run(y_third, 1)],
        (4, 0): [run(pairs, 3)],
        (4, 3): [a(2, 0), a(2, 3), a(2, 1), bb(2, 2), a(2, 2)],
        (4, 2): [run(y_mid, 1), run(y_final, 0)],
        (4, 5): [run(y_final, 1)],
        (6, 0): [run(pairs, 2)],
    }

    def later(step, point, work):
        if step < STEPS:
            plan.setdefault((step, point), []).append(work)

    for b in range(STEPS):
        if b % 2 == 0:
            stages = (
                (2, 1, y_second), (2, 1, x_second), (2, 4, y_third), (2, 4, x_third),
                (3, 6, y_mid), (3, 6, x_mid), (4, 2, y_final), (4, 2, x_final),
            )
        else:
            stages = (
                (1, 2, y_second), (1, 3, x_second), (1, 6, y_third), (2, 4, x_third),
                (3, 1, y_mid), (3, 2, x_mid), (3, 3, y_final), (3, 4, x_final),
            )
        if b == STEPS - 3:
            stages = tuple(((2, 6, x_third) if work is x_third else (lag, point, work)) for lag, point, work in stages)
        for lag, point, work in stages:
            if b > 1:
                later(b + lag, point, run(work, b))
    later(STEPS - 1, 6, run(y_second, STEPS - 2))
    for b in range(STEPS):
        later(b, 4, run(y_first, b))
        if b > 1:
            later(b, 5, run(x_first, b, 0))
            if b % 2 == 0:
                later(b + 1, 3, run(x_first, b, 1))
            else:
                plan.setdefault((b + 1, 1), []).insert(0, run(x_first, b, 1))

    def batch(b, carry):
        def hook(point):
            for value in range(STEPS):
                work = plan.get((value, point), [])
                if work:

                    @pl.when(b == value)
                    def _():
                        with jax.named_scope("hook%d" % point):
                            for item in work:
                                item()

        zz = (z + batch_z(b // 2)) % RING
        rows = pl.ds(pl.multiple_of((b % 2) * HALF, HALF), HALF)
        hook(0)

        for i in range(HID // TILE):

            @pl.when(b == 0)
            def _():
                hidden_owners((3, 1, 2), i)

            @pl.when((b % 2 == 0) & (b > 0))
            def _():
                hidden_row(zz, i)
                if i == 0:
                    join(b + 3, 1, 3)

            if i < 2:
                hook(1 + i)
        backs(b, rows, hook)
        return carry

    lax.fori_loop(0, STEPS, batch, 0)
    join(STEPS - 1, (STEPS - 1) % 2, 3)
    final = STEPS - 1
    x_first(final, 1)
    x_second(final - 1)
    y_second(final)
    y_final(final - 3)
    x_final(final - 3)
    x_second(final)
    y_third(final - 1)
    x_third(final - 1)
    y_final(final - 2)
    x_final(final - 2)
    y_third(final)
    x_third(final)
    for b in (final - 1, final):
        y_final(b)
        x_final(b)
    with jax.named_scope("last"):
        for part, ref in enumerate((zy, zx)):
            for h in range(2):
                rows, lanes = pl.ds(h * HALF, HALF), pl.ds(part * LANES, LANES)
                total = kept[rows, lanes]
                for b in range(2 + h, STEPS, 2):
                    z_copy(b, part).wait()
                    total = total + ref[b - 2].astype(f32)
                out[rows, lanes] = total.astype(bf16)
    with jax.named_scope("leave"):
        block = OWN * QUART
        small = sum(size for key, size in sent.items() if key[0] in ("fx", "fz"))
        blocks = (sum(sent.values()) - small) // block
        assert blocks * block + small == sum(sent.values())
        assert blocks == 60 and small == 15 * INFO * OWN
        for group, ref in enumerate((xall.at[:, pl.ds(0, 15)], facts.at[pl.ds(0, 15)])):
            pltpu.make_async_remote_copy(
                src_ref=ref, dst_ref=ref, send_sem=gsem.at[group], recv_sem=rsem.at[0],
                device_id=device(0, 0, 0, other), device_id_type=MESH,
            ).wait_send()


def local(tokens, scores, expert_ids, gate_weight, up_weight, down_weight):
    weights = [w.reshape(HID, WIDTH) for w in (gate_weight, up_weight, down_weight)]
    dma = pltpu.SemaphoreType.DMA
    count = len(IDS)
    scratch = [
        (HID, WIDTH), (HID, WIDTH), (HID, WIDTH),
        (RING, OWN, HID), (RING * RING, OWN, HID),
        (4, 4, BATCH, CHUNK), (4, 2, BATCH, CHUNK), (2, 4, BATCH, CHUNK),
        (2, 2, 128, CHUNK), (6, 2, 128, LANES),
        (2, 2, BATCH, CHUNK), (6, 2, BATCH, LANES),
        (2, BATCH, CHUNK), (6, BATCH, LANES),
        (2, 2, 32, CHUNK), (6, 2, 32, LANES), (2, 2, HALF, CHUNK), (6, 2, HALF, LANES), (3, 3, HALF, LANES),
        (6, 2, 4, 32, LANES), (6, 2, 4, HALF, LANES),
        (6, 4, HALF, LANES), (6, 2, 32, LANES), (6, 2, HALF, LANES), (3, 3, HALF, LANES),
    ]
    return pl.pallas_call(
        kernel,
        out_shape=jax.ShapeDtypeStruct((OWN, CHUNK), bf16),
        in_specs=[pl.BlockSpec(memory_space=pl.ANY)] * 6,
        out_specs=pl.BlockSpec(memory_space=pltpu.VMEM),
        scratch_shapes=[
            pltpu.VMEM((2, 16, OWN, 2 * QUART), bf16), pltpu.VMEM((16, INFO, OWN), bf16),
            pltpu.VMEM((TOP, OWN), f32), pltpu.VMEM((TOP, OWN), jnp.int32),
        ]
        + [pltpu.VMEM(shape, bf16) for shape in scratch]
        + [pltpu.VMEM((OWN, CHUNK), f32)]
        + [pltpu.VMEM((6, HALF, LANES), bf16)] * 4
        + [dma((9,)), dma((2,)), dma((count + 11,)), dma((2, 4)), dma((2, 4)), dma((94,)), dma((94,))],
        compiler_params=pltpu.CompilerParams(
            collective_id=0, has_side_effects=True, vmem_limit_bytes=67043328
        ),
    )(tokens, scores.T, expert_ids.T, *weights)


def solution(mesh):
    in_specs = (
        P("expert", None),
        P("expert", None),
        P("expert", None),
        P("expert", "tensor", None),
        P("expert", "tensor", None),
        P("expert", "tensor", None),
    )
    out_specs = P("expert", "tensor")
    return jax.shard_map(local, mesh=mesh, in_specs=in_specs, out_specs=out_specs, check_vma=False)
```

```python
import jax
import jax.numpy as jnp
from jax import lax
from jax.experimental import pallas as pl
from jax.experimental.pallas import tpu as pltpu
from jax.sharding import PartitionSpec as P

MESH = pl.DeviceIdType.MESH
f32 = jnp.float32
bf16 = jnp.bfloat16

RING = 4
OWN = 128
WIDTH = 4096
FFS = 192
HELD = 4
QUART = 1024
FIRST = 768
INFO = 16
CHUNK = 512
TOP = 8
HID = HELD * FFS
TILE = 256
LANES = 256
HALF = OWN // 2
STEPS = 2 * RING
BATCH = RING * HALF
ORDER = (2, 1, 3, 0)
NT = (((1,), (1,)), ((), ()))


def distance(kind, dz, dx):
    if kind == 0:
        return dx if dz == 0 else dz
    return dz if dx == 0 else dx


def transfer_ids():
    ids = {}
    for kind in range(2):
        for dz in range(RING):
            for dx in range(RING):
                if dz == 0:
                    continue
                ids[kind, dz, dx] = len(ids)
    for dz in range(RING):
        ids[dz] = len(ids)
    return ids


IDS = transfer_ids()


def scoped(name):
    def wrap(body):
        def inner(*args):
            with jax.named_scope(name):
                return body(*args)

        return inner

    return wrap


def kernel(
    tokens, scores, ids, wg_in, wu_in, wd_in, out,
    xall, facts, score_buf, ids_buf, wg, wu, wd, hid, gx, mine, chunk, dgot,
    y1a, y1b, y2a, y2b, tota, totb, xs1a, xs1b, xs2a, xs2b, xs3, xg1, xg2, wrow, ys1, ys2, ys3, kept, leave_y, leave_x, zy, zx,
    lsem, gsem, rsem, d_s, d_r, q_s, q_r,
):
    me = lax.axis_index("expert")
    rank = lax.axis_index("tensor")
    z, x = me // RING, me % RING
    y, c = rank // 2, rank % 2
    other = 1 - c

    def device(dz, dx, dy, core):
        return (((z + dz) % RING) * RING + (x + dx) % RING, ((y + dy) % RING) * 2 + core)

    peers = [device(0, 0, 0, other)]
    for step in (1, 3, 2):
        peers += [device(0, step, 0, c), device(step, 0, 0, c)]
    peers += [device(0, 0, step, c) for step in (1, 3, 2)]
    barrier = pltpu.get_barrier_semaphore()
    for peer in peers:
        pl.semaphore_signal(barrier, inc=1, device_id=peer, device_id_type=MESH)

    loads = []

    def load(src, dst):
        copy = pltpu.make_async_copy(src, dst, lsem.at[len(loads)])
        loads.append(copy)
        copy.start()
        return copy

    fact_loads = [load(scores, score_buf), load(ids, ids_buf)]
    own_loads = []
    for half in range(2):
        own_loads.append(load(tokens.at[:, pl.ds(half * 2 * QUART, 2 * QUART)], xall.at[half, me]))

    def view(kind, half, dz, dx, part):
        owner = ((z + dz) % RING) * RING + (x + dx) % RING
        rows = {"h0": pl.ds(0, 64), "h1": pl.ds(64, 64), "f": pl.ds(0, OWN)}[part]
        lanes = pl.ds(FIRST, 2 * QUART - FIRST) if kind else pl.ds(0, FIRST)
        return xall.at[half, owner, rows, lanes]

    sent = {}

    def push(key, ref, to, ident, group=0):
        copy = pltpu.make_async_remote_copy(
            src_ref=ref, dst_ref=ref, send_sem=gsem.at[group], recv_sem=rsem.at[ident],
            device_id=to, device_id_type=MESH,
        )
        sent[key] = ref.size
        copy.start()

    def pull(ref, ident):
        pltpu.make_async_remote_copy(
            src_ref=ref, dst_ref=ref, send_sem=gsem.at[0], recv_sem=rsem.at[ident],
            device_id=device(0, 0, 0, other), device_id_type=MESH,
        ).wait_recv()

    def send(kind, dz, dx, part, tz, tx):
        ident = IDS[kind, (dz - tz) % RING, (dx - tx) % RING]
        push((kind, dz, dx, part, tz, tx), view(kind, c, dz, dx, part), device(tz, tx, 0, c), ident)

    def pair(kind, dz, dx):
        push((kind, dz, dx), view(kind, c, dz, dx, "f"), device(0, 0, 0, other), IDS[dz])

    def pairs(dz):
        count = RING if dz else RING - 1
        pull(xall.at[other, pl.ds(0, count)], IDS[dz])

    def along(kind, first, step):
        if (kind == 0) == first:
            return (0, step)
        return (step, 0)

    def arrive(kind, first, dz, dx):
        d = distance(kind, dz, dx)
        pull(view(kind, c, dz, dx, "f"), IDS[kind, dz, dx])
        if d != 2:
            if d == 3:
                send(kind, dz, dx, "h0", *along(kind, first, 1))
            else:
                send(kind, dz, dx, "h1", *along(kind, first, 3))
        pair(kind, dz, dx)

    def spread(kind, first, dz, dx):
        for step in (1, 3):
            send(kind, dz, dx, "f", *along(kind, first, step))

    queue_ids = {}

    def queued(key, src, dst, to):
        ident = queue_ids.setdefault(key, len(queue_ids))
        return pltpu.make_async_remote_copy(
            src_ref=src, dst_ref=dst, send_sem=q_s.at[ident], recv_sem=q_r.at[ident],
            device_id=to, device_id_type=MESH,
        )

    def begin(copies):
        for copy in copies:
            copy.start()

    def finish(copies):
        for copy in copies:
            copy.wait()

    def batch_z(b):
        return (b * (b + 1) // 2) % RING

    def wide(b):
        return CHUNK if b < 2 else LANES

    def y1(b):
        return y1a.at[b] if b < 2 else y1b.at[b - 2]

    def y2(b):
        return y2a.at[b] if b < 2 else y2b.at[b - 2]

    def tot(b):
        return tota.at[b] if b < 2 else totb.at[b - 2]

    def xs1(b):
        return xs1a.at[b] if b < 2 else xs1b.at[b - 2]

    def xs2(b):
        return xs2a.at[b] if b < 2 else xs2b.at[b - 2]

    def owner_rows(dx, start, size):
        return pl.ds(pl.multiple_of(((x + dx) % RING) * HALF + start, 32), size)

    def y_copies(b, stage):
        lanes = pl.ds(0, wide(b))
        if stage == 0:
            pieces = [(mine.at[b % 4, 0, pl.ds(n * 128, 128), lanes], y1(b).at[n]) for n in range(2)]
        else:
            pieces = [(mine.at[b % 4, 1 + n, :, lanes], y2(b).at[n]) for n in range(2)]
        return [
            queued(("y", b if b < 2 else 2 + b % 2, stage, n), src, dst, device(0, 0, (1, 3)[n], c)) for n, (src, dst) in enumerate(pieces)
        ]

    def direct(b):
        return b >= STEPS - 4

    def y_last(b, stage):
        if direct(b):
            return [
                queued(("ydirect", b, d), tot(b).at[owner_rows(d, 0, HALF)], xs3.at[b - STEPS + 4, d - 1], device(0, d, 0, c))
                for d in (2, 1, 3)
            ]
        if stage == 0:
            pieces = [(tot(b).at[owner_rows(2, 32 * n, 32)], xs1(b).at[n]) for n in range(2)]
        else:
            pieces = [(tot(b).at[owner_rows((1, 3)[n], 0, HALF)], xs2(b).at[n]) for n in range(2)]
        return [
            queued(("ylast", b if b < 2 else 2 + b % 2, stage, n), src, dst, device(0, (1, 3)[n], 0, c)) for n, (src, dst) in enumerate(pieces)
        ]

    @scoped("y_first")
    def y_first(b):
        begin(y_copies(b, 0))

    @scoped("y_second")
    def y_second(b):
        finish(y_copies(b, 0))
        lanes = pl.ds(0, wide(b))
        for n in range(2):
            rows = pl.ds(n * 128, 128)
            mine[b % 4, 1 + n, rows, lanes] = mine[b % 4, 1 + n, rows, lanes] + y1(b)[n]
        begin(y_copies(b, 1))

    @scoped("y_third")
    def y_third(b):
        finish(y_copies(b, 1))
        tot(b)[...] = (
            mine[b % 4, 3, :, pl.ds(0, wide(b))].astype(f32) + y2(b)[0].astype(f32) + y2(b)[1].astype(f32)
        ).astype(bf16)
        begin(y_last(b, 0))

    @scoped("y_mid")
    def y_mid(b):
        finish(y_last(b, 0))
        for n in range(2):
            rows = owner_rows((1, 3)[n], 32 * n, 32)
            tot(b)[rows] = (tot(b)[rows].astype(f32) + xs1(b)[n].astype(f32)).astype(bf16)
        begin(y_last(b, 1))

    def z_copy(b, part):
        src, dst = ((leave_y, zy), (leave_x, zx))[part]
        return queued(("z", b, part), src.at[b - 2], dst.at[b - 2], device(batch_z(b // 2), 0, 0, c))

    @scoped("y_final")
    def y_final(b):
        finish(y_last(b, 1))
        value = tot(b)[owner_rows(0, 0, HALF)].astype(f32)
        for ref in [xs3.at[b - STEPS + 4, n] for n in range(3)] if direct(b) else [xs2(b).at[n] for n in range(2)]:
            value = value + ref[...].astype(f32)
        if b < 2:
            kept[pl.ds(b * HALF, HALF)] = value
        else:
            leave_y[b - 2] = value.astype(bf16)
            z_copy(b, 0).start()

    upper = pl.ds(LANES, LANES)

    def x_copies(b, stage, p):
        both = pl.ds(2 * p, 2)
        if stage == 0:
            pieces = [
                (mine.at[b % 4, both, owner_rows(2, 32 * n, 32), upper], xg1.at[b - 2, n, both]) for n in range(2)
            ]
        else:
            pieces = [
                (mine.at[b % 4, both, owner_rows((1, 3)[n], 0, HALF), upper], xg2.at[b - 2, n, both])
                for n in range(2)
            ]
        return [
            queued(("x", b % 2 + b // (STEPS - 1), stage, n, p), src, dst, device(0, (1, 3)[n], 0, c))
            for n, (src, dst) in enumerate(pieces)
        ]

    def x_last(b, stage):
        if direct(b):
            return [
                queued(("xdirect", b, i), wrow.at[b - 2, i], ys3.at[b - STEPS + 4, i], device(0, 0, ORDER[i], c)) for i in range(3)
            ]
        if stage == 0:
            pieces = [(wrow.at[b - 2, 0, pl.ds(32 * n, 32)], ys1.at[b - 2, n]) for n in range(2)]
        else:
            pieces = [(wrow.at[b - 2, 1 + n], ys2.at[b - 2, n]) for n in range(2)]
        return [
            queued(("xlast", b % 2, stage, n), src, dst, device(0, 0, (1, 3)[n], c)) for n, (src, dst) in enumerate(pieces)
        ]

    @scoped("x_first")
    def x_first(b, p):
        begin(x_copies(b, 0, p))

    @scoped("x_second")
    def x_second(b):
        for p in range(2):
            finish(x_copies(b, 0, p))
            for n in range(2):
                rows = owner_rows((1, 3)[n], 32 * n, 32)
                for i in (2 * p, 2 * p + 1):
                    mine[b % 4, i, rows, upper] = mine[b % 4, i, rows, upper] + xg1[b - 2, n, i]
            begin(x_copies(b, 1, p))

    @scoped("x_third")
    def x_third(b):
        rows = owner_rows(0, 0, HALF)
        for p in range(2):
            finish(x_copies(b, 1, p))
            for i in (2 * p, 2 * p + 1):
                wrow[b - 2, i] = (
                    mine[b % 4, i, rows, upper].astype(f32)
                    + xg2[b - 2, 0, i].astype(f32)
                    + xg2[b - 2, 1, i].astype(f32)
                ).astype(bf16)
            if p == direct(b):
                begin(x_last(b, 0))

    @scoped("x_mid")
    def x_mid(b):
        finish(x_last(b, 0))
        for n in range(2):
            rows = pl.ds(32 * n, 32)
            wrow[b - 2, 1 + n, rows] = (
                wrow[b - 2, 1 + n, rows].astype(f32) + ys1[b - 2, n].astype(f32)
            ).astype(bf16)
        begin(x_last(b, 1))

    @scoped("x_final")
    def x_final(b):
        finish(x_last(b, 1))
        value = wrow[b - 2, 3].astype(f32)
        for ref in [ys3.at[b - STEPS + 4, n] for n in range(3)] if direct(b) else [ys2.at[b - 2, n] for n in range(2)]:
            value = value + ref[...].astype(f32)
        leave_x[b - 2] = value.astype(bf16)
        z_copy(b, 1).start()

    @scoped("gates")
    def gates(zz):
        member = lax.broadcasted_iota(jnp.int32, (8, HID), 0)
        unit = lax.broadcasted_iota(jnp.int32, (8, HID), 1)
        expand = jnp.where((unit >= member * FFS) & (unit < member * FFS + FFS), 1.0, 0.0).astype(bf16)
        for o in range(RING):
            about = facts[zz * RING + o].astype(f32)
            named, values = about[0:8], about[8:16]
            found = [
                jnp.sum(jnp.where(named == (me * HELD + j).astype(f32), values, 0.0), axis=0, keepdims=True)
                for j in range(HELD)
            ]
            held = jnp.concatenate(found + [jnp.zeros((8 - HELD, OWN), f32)], axis=0).astype(bf16)
            gx[zz * RING + o] = lax.dot_general(
                held, expand, (((0,), (0,)), ((), ())), preferred_element_type=f32
            ).astype(bf16)

    @scoped("hidden")
    def hidden(load_block, load_scale, count, i):
        units = pl.ds(i * TILE, TILE)
        gate = jnp.zeros((count * OWN, TILE), f32)
        up = jnp.zeros((count * OWN, TILE), f32)
        for half in range(2):
            for q in range(2):
                block = load_block(half, pl.ds(q * QUART, QUART))
                columns = pl.ds((half * 2 + q) * QUART, QUART)
                gate = gate + lax.dot_general(block, wg[units, columns], NT, preferred_element_type=f32)
                up = up + lax.dot_general(block, wu[units, columns], NT, preferred_element_type=f32)
        scale = load_scale(units).astype(f32)
        return (gate * (1.0 / (1.0 + jnp.exp(-gate))) * up * scale).astype(bf16)

    def hidden_row(zz, i):
        owners = pl.ds(zz * RING, RING)
        value = hidden(
            lambda half, lanes: xall[half, owners, :, lanes].reshape(RING * OWN, QUART),
            lambda units: gx[owners, :, units].reshape(RING * OWN, TILE),
            RING,
            i,
        )
        hid[:, :, pl.ds(i * TILE, TILE)] = value.reshape(RING, OWN, TILE)

    def hidden_owners(steps, i):
        places = [(x + d) % RING for d in steps]
        owners = [z * RING + place for place in places]
        value = hidden(
            lambda half, lanes: jnp.concatenate([xall[half, o, :, lanes] for o in owners], axis=0),
            lambda units: jnp.concatenate([gx[o, :, units] for o in owners], axis=0),
            len(owners),
            i,
        )
        for n, place in enumerate(places):
            hid[place, :, pl.ds(i * TILE, TILE)] = value[n * OWN : (n + 1) * OWN]

    def d_copy(s, i):
        return pltpu.make_async_remote_copy(
            src_ref=chunk.at[i, other], dst_ref=dgot.at[s, i], send_sem=d_s.at[s, i], recv_sem=d_r.at[s, i],
            device_id=device(0, 0, 0, other), device_id_type=MESH,
        )

    def down(rows, s, i):
        with jax.named_scope("down"):
            column = pl.multiple_of(((y + ORDER[i]) % RING) * 2 * CHUNK, CHUNK)
            value = jnp.dot(hid[:, rows, :].reshape(BATCH, HID), wd[:, pl.ds(column, 2 * CHUNK)], preferred_element_type=f32).astype(bf16)
            chunk[i, 0] = value[:, :CHUNK]
            chunk[i, 1] = value[:, CHUNK:]
            d_copy(s, i).start()

    def join(b, s, i):
        with jax.named_scope("join"):
            d_copy(s, i).wait()
        mine[b % 4, i] = chunk[i, c] + dgot[s, i]

    def backs(b, rows, hook):
        s = b % 2
        down(rows, s, 0)

        @pl.when(s == 1)
        def _():
            join(b + 3, 0, 3)

        hook(3)
        down(rows, s, 1)
        down(rows, s, 2)
        join(b, s, 0)
        hook(4)
        down(rows, s, 3)
        join(b, s, 1)
        hook(5)
        join(b, s, 2)
        hook(6)

    def fact_copies(stage):
        if stage == 0:
            for d in (2, 1, 3):
                push(("fx", d), facts.at[me], device(0, d, 0, c), len(IDS), 1)
        else:
            for d in (2, 1, 3):
                push(("fz", d), facts.at[pl.ds(z * RING, RING)], device(d, 0, 0, c), len(IDS) + 1, 1)

    def fact_waits(stage):
        pull(facts.at[pl.ds(0, 12 if stage else 3)], len(IDS) + stage)

    finish(fact_loads)
    lifted = jnp.exp(score_buf[...])
    gate_values = (lifted / jnp.sum(lifted, axis=0, keepdims=True)).astype(bf16).astype(f32)
    facts[me] = jnp.concatenate([ids_buf[...].astype(f32), gate_values], axis=0).astype(bf16)

    with jax.named_scope("enter"):
        pl.semaphore_wait(barrier, len(peers))
    with jax.named_scope("own"):
        finish(own_loads)
    parity = y % 2

    def own_view(dx, h, lanes):
        owner = z * RING + (x + dx) % RING
        rows = pl.ds(0, OWN) if h is None else pl.ds(64 * h, 64)
        return xall.at[c, owner, rows, pl.ds(pl.multiple_of(lanes * QUART, QUART), QUART)]

    own_ids = {}

    def own_send(axis, dx, h, step):
        key = ("x", (dx - step) % RING, h) if axis == "x" else ("y", dx)
        ident = own_ids.setdefault(key, len(IDS) + 2 + len(own_ids))
        to = device(0, step, 0, c) if axis == "x" else device(0, 0, step, c)
        push((axis, dx, h, step), own_view(dx, h, parity), to, ident)

    def own_got(axis, dx, h):
        if axis == "x":
            pull(own_view(dx, h, parity), own_ids["x", dx, h])
        else:
            pull(own_view(dx, None, 1 - parity), own_ids["y", dx])

    def sideways(dx, h):
        own_send("y", dx, h, (1, 3)[h])

    fact_copies(0)
    own_send("x", 0, 0, 1)
    own_send("x", 0, 1, 3)
    own_send("x", 0, 1, 1)
    own_send("x", 0, 0, 3)
    spread(1, True, 0, 0)
    fact_waits(0)
    fact_copies(1)
    spread(0, False, 0, 0)

    weight_loads = [load(wg_in, wg), load(wu_in, wu), load(wd_in, wd)]
    with jax.named_scope("ox1"):
        own_got("x", 3, 0)
        own_send("x", 3, 0, 1)
        sideways(3, 0)
        own_got("x", 1, 1)
        own_send("x", 1, 1, 3)
        sideways(1, 1)
    finish(weight_loads[:2])
    gates(z)
    hidden_owners((0,), 0)
    with jax.named_scope("ox2"):
        own_got("x", 3, 1)
        sideways(3, 1)
        own_got("x", 1, 0)
        sideways(1, 0)
    with jax.named_scope("bz"):
        arrive(1, True, 3, 0)
        arrive(1, True, 1, 0)
    with jax.named_scope("ox3"):
        own_got("x", 2, 0)
        sideways(2, 0)
        own_got("x", 2, 1)
        sideways(2, 1)
        spread(1, False, 1, 0)
        spread(1, False, 3, 0)
    with jax.named_scope("fz"):
        fact_waits(1)
    hidden_owners((0,), 1)
    hidden_owners((0,), 2)
    for dx in (3, 1, 2):
        with jax.named_scope("oy%d" % dx):
            own_got("y", dx, 0)
            spread(0, False, 0, dx)
            pair(0, 0, dx)
            pair(1, 0, dx)
        if dx != 2:
            gates((z + dx) % RING)
    with jax.named_scope("pairs"):
        pairs(0)
    finish(weight_loads[2:])

    def a(dz, dx):
        return lambda: arrive(0, False, dz, dx)

    def bb(dz, dx):
        return lambda: arrive(1, dx == 0, dz, dx)

    def run(f, *args):
        return lambda: f(*args)

    def xf(b, i):
        return run(x_first, b, i)

    plan = {
        (0, 0): [a(1, 0), a(3, 0)],
        (0, 2): [bb(1, 3), bb(1, 1)],
        (0, 4): [a(3, 3), a(1, 3)],
        (1, 3): [a(3, 1), a(1, 1), bb(3, 3), bb(3, 1)],
        (1, 4): [bb(2, 0), run(spread, 1, False, 2, 0)],
        (2, 0): [run(gates, (z + 2) % RING), a(1, 2), a(3, 2), bb(1, 2), run(pairs, 1), run(y_second, 0)],
        (2, 1): [run(y_second, 1)],
        (2, 4): [run(y_third, 0)],
        (3, 0): [bb(3, 2)],
        (2, 6): [bb(2, 3), bb(2, 1)],
        (3, 6): [run(y_mid, 0), run(y_third, 1)],
        (4, 0): [run(pairs, 3)],
        (4, 3): [a(2, 0), a(2, 3), a(2, 1), bb(2, 2), a(2, 2), run(y_mid, 1)],
        (5, 3): [run(y_final, 0)],
        (5, 6): [run(y_final, 1)],
        (6, 0): [run(pairs, 2)],
    }

    def later(step, point, work):
        if step < STEPS:
            plan.setdefault((step, point), []).append(work)

    for b in range(STEPS):
        if b % 2 == 0:
            stages = (
                (2, 1, y_second), (2, 1, x_second), (2, 4, y_third), (2, 4, x_third),
                (3, 6, y_mid), (3, 6, x_mid), (4, 2, y_final), (4, 2, x_final),
            )
        else:
            stages = (
                (1, 2, y_second), (1, 3, x_second), (1, 6, y_third), (2, 4, x_third),
                (3, 1, y_mid), (3, 2, x_mid), (3, 3, y_final), (3, 4, x_final),
            )
        if b == STEPS - 3:
            stages = tuple(((2, 6, x_third) if work is x_third else (lag, point, work)) for lag, point, work in stages)
        if b == 2:
            stages = tuple(((2, 2, x_second) if work is x_second else (lag, point, work)) for lag, point, work in stages)
        if b >= STEPS - 4:
            stages = tuple(item for item in stages if item[2] not in (y_mid, x_mid))
        for lag, point, work in stages:
            if b > 1:
                later(b + lag, point, run(work, b))
    later(STEPS - 1, 6, run(y_second, STEPS - 2))
    for b in range(STEPS):
        later(b, 4, run(y_first, b))
        if b > 1:
            later(b, 5, run(x_first, b, 0))
            if b % 2 == 0:
                later(b + 1, 3, run(x_first, b, 1))
            else:
                plan.setdefault((b + 1, 1), []).insert(0, run(x_first, b, 1))

    def batch(b, carry):
        def hook(point):
            for value in range(STEPS):
                work = plan.get((value, point), [])
                if work:

                    @pl.when(b == value)
                    def _():
                        with jax.named_scope("hook%d" % point):
                            for item in work:
                                item()

        zz = (z + batch_z(b // 2)) % RING
        rows = pl.ds(pl.multiple_of((b % 2) * HALF, HALF), HALF)
        hook(0)

        for i in range(HID // TILE):

            @pl.when(b == 0)
            def _():
                hidden_owners((3, 1, 2), i)

            @pl.when((b % 2 == 0) & (b > 0))
            def _():
                hidden_row(zz, i)
                if i == 0:
                    join(b + 3, 1, 3)

            if i < 2:
                hook(1 + i)
        backs(b, rows, hook)
        return carry

    lax.fori_loop(0, STEPS, batch, 0)
    join(STEPS - 1, (STEPS - 1) % 2, 3)
    final = STEPS - 1
    x_first(final, 1)
    x_second(final - 1)
    y_second(final)
    y_final(final - 3)
    x_final(final - 3)
    x_second(final)
    y_third(final - 1)
    x_third(final - 1)
    y_final(final - 2)
    x_final(final - 2)
    y_third(final)
    x_third(final)
    for b in (final - 1, final):
        y_final(b)
        x_final(b)
    with jax.named_scope("last"):
        for part, ref in enumerate((zy, zx)):
            for h in range(2):
                rows, lanes = pl.ds(h * HALF, HALF), pl.ds(part * LANES, LANES)
                total = kept[rows, lanes]
                for b in range(2 + h, STEPS, 2):
                    z_copy(b, part).wait()
                    total = total + ref[b - 2].astype(f32)
                out[rows, lanes] = total.astype(bf16)
    with jax.named_scope("leave"):
        block = OWN * QUART
        small = sum(size for key, size in sent.items() if key[0] in ("fx", "fz"))
        blocks = (sum(sent.values()) - small) // block
        assert blocks * block + small == sum(sent.values())
        assert blocks == 60 and small == 15 * INFO * OWN
        for group, ref in enumerate((xall.at[:, pl.ds(0, 15)], facts.at[pl.ds(0, 15)])):
            pltpu.make_async_remote_copy(
                src_ref=ref, dst_ref=ref, send_sem=gsem.at[group], recv_sem=rsem.at[0],
                device_id=device(0, 0, 0, other), device_id_type=MESH,
            ).wait_send()


def local(tokens, scores, expert_ids, gate_weight, up_weight, down_weight):
    weights = [w.reshape(HID, WIDTH) for w in (gate_weight, up_weight, down_weight)]
    dma = pltpu.SemaphoreType.DMA
    count = len(IDS)
    scratch = [
        (HID, WIDTH), (HID, WIDTH), (HID, WIDTH),
        (RING, OWN, HID), (RING * RING, OWN, HID),
        (4, 4, BATCH, CHUNK), (4, 2, BATCH, CHUNK), (2, 4, BATCH, CHUNK),
        (2, 2, 128, CHUNK), (6, 2, 128, LANES),
        (2, 2, BATCH, CHUNK), (6, 2, BATCH, LANES),
        (2, BATCH, CHUNK), (6, BATCH, LANES),
        (2, 2, 32, CHUNK), (6, 2, 32, LANES), (2, 2, HALF, CHUNK), (6, 2, HALF, LANES), (4, 3, HALF, LANES),
        (6, 2, 4, 32, LANES), (6, 2, 4, HALF, LANES),
        (6, 4, HALF, LANES), (6, 2, 32, LANES), (6, 2, HALF, LANES), (4, 3, HALF, LANES),
    ]
    return pl.pallas_call(
        kernel,
        out_shape=jax.ShapeDtypeStruct((OWN, CHUNK), bf16),
        in_specs=[pl.BlockSpec(memory_space=pl.ANY)] * 6,
        out_specs=pl.BlockSpec(memory_space=pltpu.VMEM),
        scratch_shapes=[
            pltpu.VMEM((2, 16, OWN, 2 * QUART), bf16), pltpu.VMEM((16, INFO, OWN), bf16),
            pltpu.VMEM((TOP, OWN), f32), pltpu.VMEM((TOP, OWN), jnp.int32),
        ]
        + [pltpu.VMEM(shape, bf16) for shape in scratch]
        + [pltpu.VMEM((OWN, CHUNK), f32)]
        + [pltpu.VMEM((6, HALF, LANES), bf16)] * 4
        + [dma((9,)), dma((2,)), dma((count + 11,)), dma((2, 4)), dma((2, 4)), dma((100,)), dma((100,))],
        compiler_params=pltpu.CompilerParams(
            collective_id=0, has_side_effects=True, vmem_limit_bytes=67043328
        ),
    )(tokens, scores.T, expert_ids.T, *weights)


def solution(mesh):
    in_specs = (
        P("expert", None),
        P("expert", None),
        P("expert", None),
        P("expert", "tensor", None),
        P("expert", "tensor", None),
        P("expert", "tensor", None),
    )
    out_specs = P("expert", "tensor")
    return jax.shard_map(local, mesh=mesh, in_specs=in_specs, out_specs=out_specs, check_vma=False)
```

```python
import jax
import jax.numpy as jnp
from jax import lax
from jax.experimental import pallas as pl
from jax.experimental.pallas import tpu as pltpu
from jax.sharding import PartitionSpec as P

MESH = pl.DeviceIdType.MESH
f32 = jnp.float32
bf16 = jnp.bfloat16

RING = 4
OWN = 128
WIDTH = 4096
FFS = 192
HELD = 4
QUART = 1024
FIRST = 768
INFO = 16
CHUNK = 512
TOP = 8
HID = HELD * FFS
TILE = 256
LANES = 256
HALF = OWN // 2
STEPS = 2 * RING
BATCH = RING * HALF
ORDER = (2, 1, 3, 0)
NT = (((1,), (1,)), ((), ()))


def distance(kind, dz, dx):
    if kind == 0:
        return dx if dz == 0 else dz
    return dz if dx == 0 else dx


def transfer_ids():
    ids = {}
    for kind in range(2):
        for dz in range(RING):
            for dx in range(RING):
                if dz == 0:
                    continue
                ids[kind, dz, dx] = len(ids)
    for dz in range(RING):
        ids[dz] = len(ids)
    return ids


IDS = transfer_ids()


def scoped(name):
    def wrap(body):
        def inner(*args):
            with jax.named_scope(name):
                return body(*args)

        return inner

    return wrap


def kernel(
    tokens, scores, ids, wg_in, wu_in, wd_in, out,
    xall, facts, score_buf, ids_buf, wg, wu, wd, hid, gx, mine, chunk, dgot,
    y1a, y1b, y2a, y2b, tota, totb, xs1a, xs1b, xs2a, xs2b, xs3, xg1, xg2, wrow, ys1, ys2, ys3, kept, leave_y, leave_x, zy, zx,
    lsem, gsem, rsem, d_s, d_r, q_s, q_r,
):
    me = lax.axis_index("expert")
    rank = lax.axis_index("tensor")
    z, x = me // RING, me % RING
    y, c = rank // 2, rank % 2
    other = 1 - c

    def device(dz, dx, dy, core):
        return (((z + dz) % RING) * RING + (x + dx) % RING, ((y + dy) % RING) * 2 + core)

    peers = [device(0, 0, 0, other)]
    for step in (1, 3, 2):
        peers += [device(0, step, 0, c), device(step, 0, 0, c)]
    peers += [device(0, 0, step, c) for step in (1, 3, 2)]
    barrier = pltpu.get_barrier_semaphore()
    for peer in peers:
        pl.semaphore_signal(barrier, inc=1, device_id=peer, device_id_type=MESH)

    loads = []

    def load(src, dst):
        copy = pltpu.make_async_copy(src, dst, lsem.at[len(loads)])
        loads.append(copy)
        copy.start()
        return copy

    fact_loads = [load(scores, score_buf), load(ids, ids_buf)]
    own_loads = []
    for half in range(2):
        own_loads.append(load(tokens.at[:, pl.ds(half * 2 * QUART, 2 * QUART)], xall.at[half, me]))

    def view(kind, half, dz, dx, part):
        owner = ((z + dz) % RING) * RING + (x + dx) % RING
        rows = {"h0": pl.ds(0, 64), "h1": pl.ds(64, 64), "f": pl.ds(0, OWN)}[part]
        lanes = pl.ds(FIRST, 2 * QUART - FIRST) if kind else pl.ds(0, FIRST)
        return xall.at[half, owner, rows, lanes]

    sent = {}

    def push(key, ref, to, ident, group=0):
        copy = pltpu.make_async_remote_copy(
            src_ref=ref, dst_ref=ref, send_sem=gsem.at[group], recv_sem=rsem.at[ident],
            device_id=to, device_id_type=MESH,
        )
        sent[key] = ref.size
        copy.start()

    def pull(ref, ident):
        pltpu.make_async_remote_copy(
            src_ref=ref, dst_ref=ref, send_sem=gsem.at[0], recv_sem=rsem.at[ident],
            device_id=device(0, 0, 0, other), device_id_type=MESH,
        ).wait_recv()

    def send(kind, dz, dx, part, tz, tx):
        ident = IDS[kind, (dz - tz) % RING, (dx - tx) % RING]
        push((kind, dz, dx, part, tz, tx), view(kind, c, dz, dx, part), device(tz, tx, 0, c), ident)

    def pair(kind, dz, dx):
        push((kind, dz, dx), view(kind, c, dz, dx, "f"), device(0, 0, 0, other), IDS[dz])

    def pairs(dz):
        count = RING if dz else RING - 1
        pull(xall.at[other, pl.ds(0, count)], IDS[dz])

    def along(kind, first, step):
        if (kind == 0) == first:
            return (0, step)
        return (step, 0)

    def arrive(kind, first, dz, dx):
        d = distance(kind, dz, dx)
        pull(view(kind, c, dz, dx, "f"), IDS[kind, dz, dx])
        if d != 2:
            if d == 3:
                send(kind, dz, dx, "h0", *along(kind, first, 1))
            else:
                send(kind, dz, dx, "h1", *along(kind, first, 3))
        pair(kind, dz, dx)

    def spread(kind, first, dz, dx):
        for step in (1, 3):
            send(kind, dz, dx, "f", *along(kind, first, step))

    queue_ids = {}

    def queued(key, src, dst, to):
        ident = queue_ids.setdefault(key, len(queue_ids))
        return pltpu.make_async_remote_copy(
            src_ref=src, dst_ref=dst, send_sem=q_s.at[ident], recv_sem=q_r.at[ident],
            device_id=to, device_id_type=MESH,
        )

    def begin(copies):
        for copy in copies:
            copy.start()

    def finish(copies):
        for copy in copies:
            copy.wait()

    def batch_z(b):
        return (b * (b + 1) // 2) % RING

    def wide(b):
        return CHUNK if b < 2 else LANES

    def y1(b):
        return y1a.at[b] if b < 2 else y1b.at[b - 2]

    def y2(b):
        return y2a.at[b] if b < 2 else y2b.at[b - 2]

    def tot(b):
        return tota.at[b] if b < 2 else totb.at[b - 2]

    def xs1(b):
        return xs1a.at[b] if b < 2 else xs1b.at[b - 2]

    def xs2(b):
        return xs2a.at[b] if b < 2 else xs2b.at[b - 2]

    def owner_rows(dx, start, size):
        return pl.ds(pl.multiple_of(((x + dx) % RING) * HALF + start, 32), size)

    def y_copies(b, stage):
        lanes = pl.ds(0, wide(b))
        if stage == 0:
            pieces = [(mine.at[b % 4, 0, pl.ds(n * 128, 128), lanes], y1(b).at[n]) for n in range(2)]
        else:
            pieces = [(mine.at[b % 4, 1 + n, :, lanes], y2(b).at[n]) for n in range(2)]
        return [
            queued(("y", b if b < 2 else 2 + b % 2, stage, n), src, dst, device(0, 0, (1, 3)[n], c)) for n, (src, dst) in enumerate(pieces)
        ]

    def direct(b):
        return b >= STEPS - 4

    def y_last(b, stage):
        if direct(b):
            return [
                queued(("ydirect", b, d), tot(b).at[owner_rows(d, 0, HALF)], xs3.at[b - STEPS + 4, d - 1], device(0, d, 0, c))
                for d in (2, 1, 3)
            ]
        if stage == 0:
            pieces = [(tot(b).at[owner_rows(2, 32 * n, 32)], xs1(b).at[n]) for n in range(2)]
        else:
            pieces = [(tot(b).at[owner_rows((1, 3)[n], 0, HALF)], xs2(b).at[n]) for n in range(2)]
        return [
            queued(("ylast", b if b < 2 else 2 + b % 2, stage, n), src, dst, device(0, (1, 3)[n], 0, c)) for n, (src, dst) in enumerate(pieces)
        ]

    @scoped("y_first")
    def y_first(b):
        begin(y_copies(b, 0))

    @scoped("y_second")
    def y_second(b):
        finish(y_copies(b, 0))
        lanes = pl.ds(0, wide(b))
        for n in range(2):
            rows = pl.ds(n * 128, 128)
            mine[b % 4, 1 + n, rows, lanes] = mine[b % 4, 1 + n, rows, lanes] + y1(b)[n]
        begin(y_copies(b, 1))

    @scoped("y_third")
    def y_third(b):
        finish(y_copies(b, 1))
        tot(b)[...] = (
            mine[b % 4, 3, :, pl.ds(0, wide(b))].astype(f32) + y2(b)[0].astype(f32) + y2(b)[1].astype(f32)
        ).astype(bf16)
        begin(y_last(b, 0))

    @scoped("y_mid")
    def y_mid(b):
        finish(y_last(b, 0))
        for n in range(2):
            rows = owner_rows((1, 3)[n], 32 * n, 32)
            tot(b)[rows] = (tot(b)[rows].astype(f32) + xs1(b)[n].astype(f32)).astype(bf16)
        begin(y_last(b, 1))

    def z_copy(b, part):
        src, dst = ((leave_y, zy), (leave_x, zx))[part]
        return queued(("z", b, part), src.at[b - 2], dst.at[b - 2], device(batch_z(b // 2), 0, 0, c))

    @scoped("y_final")
    def y_final(b):
        finish(y_last(b, 1))
        value = tot(b)[owner_rows(0, 0, HALF)].astype(f32)
        for ref in [xs3.at[b - STEPS + 4, n] for n in range(3)] if direct(b) else [xs2(b).at[n] for n in range(2)]:
            value = value + ref[...].astype(f32)
        if b < 2:
            kept[pl.ds(b * HALF, HALF)] = value
        else:
            leave_y[b - 2] = value.astype(bf16)
            z_copy(b, 0).start()

    upper = pl.ds(LANES, LANES)

    def x_copies(b, stage, p):
        both = pl.ds(2 * p, 2)
        if stage == 0:
            pieces = [
                (mine.at[b % 4, both, owner_rows(2, 32 * n, 32), upper], xg1.at[b - 2, n, both]) for n in range(2)
            ]
        else:
            pieces = [
                (mine.at[b % 4, both, owner_rows((1, 3)[n], 0, HALF), upper], xg2.at[b - 2, n, both])
                for n in range(2)
            ]
        return [
            queued(("x", b % 4, stage, n, p), src, dst, device(0, (1, 3)[n], 0, c))
            for n, (src, dst) in enumerate(pieces)
        ]

    def x_last(b, stage):
        if direct(b):
            return [
                queued(("xdirect", b, i), wrow.at[b - 2, i], ys3.at[b - STEPS + 4, i], device(0, 0, ORDER[i], c)) for i in range(3)
            ]
        if stage == 0:
            pieces = [(wrow.at[b - 2, 0, pl.ds(32 * n, 32)], ys1.at[b - 2, n]) for n in range(2)]
        else:
            pieces = [(wrow.at[b - 2, 1 + n], ys2.at[b - 2, n]) for n in range(2)]
        return [
            queued(("xlast", b % 2, stage, n), src, dst, device(0, 0, (1, 3)[n], c)) for n, (src, dst) in enumerate(pieces)
        ]

    @scoped("x_first")
    def x_first(b, p):
        begin(x_copies(b, 0, p))

    @scoped("x_second")
    def x_second(b):
        for p in range(2):
            finish(x_copies(b, 0, p))
            for n in range(2):
                rows = owner_rows((1, 3)[n], 32 * n, 32)
                for i in (2 * p, 2 * p + 1):
                    mine[b % 4, i, rows, upper] = mine[b % 4, i, rows, upper] + xg1[b - 2, n, i]
            begin(x_copies(b, 1, p))

    @scoped("x_third")
    def x_third(b):
        rows = owner_rows(0, 0, HALF)
        for p in range(2):
            finish(x_copies(b, 1, p))
            for i in (2 * p, 2 * p + 1):
                wrow[b - 2, i] = (
                    mine[b % 4, i, rows, upper].astype(f32)
                    + xg2[b - 2, 0, i].astype(f32)
                    + xg2[b - 2, 1, i].astype(f32)
                ).astype(bf16)
            if p == direct(b):
                begin(x_last(b, 0))

    @scoped("x_mid")
    def x_mid(b):
        finish(x_last(b, 0))
        for n in range(2):
            rows = pl.ds(32 * n, 32)
            wrow[b - 2, 1 + n, rows] = (
                wrow[b - 2, 1 + n, rows].astype(f32) + ys1[b - 2, n].astype(f32)
            ).astype(bf16)
        begin(x_last(b, 1))

    @scoped("x_final")
    def x_final(b):
        finish(x_last(b, 1))
        value = wrow[b - 2, 3].astype(f32)
        for ref in [ys3.at[b - STEPS + 4, n] for n in range(3)] if direct(b) else [ys2.at[b - 2, n] for n in range(2)]:
            value = value + ref[...].astype(f32)
        leave_x[b - 2] = value.astype(bf16)
        z_copy(b, 1).start()

    @scoped("gates")
    def gates(zz):
        member = lax.broadcasted_iota(jnp.int32, (8, HID), 0)
        unit = lax.broadcasted_iota(jnp.int32, (8, HID), 1)
        expand = jnp.where((unit >= member * FFS) & (unit < member * FFS + FFS), 1.0, 0.0).astype(bf16)
        for o in range(RING):
            about = facts[zz * RING + o].astype(f32)
            named, values = about[0:8], about[8:16]
            found = [
                jnp.sum(jnp.where(named == (me * HELD + j).astype(f32), values, 0.0), axis=0, keepdims=True)
                for j in range(HELD)
            ]
            held = jnp.concatenate(found + [jnp.zeros((8 - HELD, OWN), f32)], axis=0).astype(bf16)
            gx[zz * RING + o] = lax.dot_general(
                held, expand, (((0,), (0,)), ((), ())), preferred_element_type=f32
            ).astype(bf16)

    @scoped("hidden")
    def hidden(load_block, load_scale, count, i):
        units = pl.ds(i * TILE, TILE)
        gate = jnp.zeros((count * OWN, TILE), f32)
        up = jnp.zeros((count * OWN, TILE), f32)
        for half in range(2):
            for q in range(2):
                block = load_block(half, pl.ds(q * QUART, QUART))
                columns = pl.ds((half * 2 + q) * QUART, QUART)
                gate = gate + lax.dot_general(block, wg[units, columns], NT, preferred_element_type=f32)
                up = up + lax.dot_general(block, wu[units, columns], NT, preferred_element_type=f32)
        scale = load_scale(units).astype(f32)
        return (gate * (1.0 / (1.0 + jnp.exp(-gate))) * up * scale).astype(bf16)

    def hidden_row(zz, i):
        owners = pl.ds(zz * RING, RING)
        value = hidden(
            lambda half, lanes: xall[half, owners, :, lanes].reshape(RING * OWN, QUART),
            lambda units: gx[owners, :, units].reshape(RING * OWN, TILE),
            RING,
            i,
        )
        hid[:, :, pl.ds(i * TILE, TILE)] = value.reshape(RING, OWN, TILE)

    def hidden_owners(steps, i):
        places = [(x + d) % RING for d in steps]
        owners = [z * RING + place for place in places]
        value = hidden(
            lambda half, lanes: jnp.concatenate([xall[half, o, :, lanes] for o in owners], axis=0),
            lambda units: jnp.concatenate([gx[o, :, units] for o in owners], axis=0),
            len(owners),
            i,
        )
        for n, place in enumerate(places):
            hid[place, :, pl.ds(i * TILE, TILE)] = value[n * OWN : (n + 1) * OWN]

    def d_copy(s, i):
        return pltpu.make_async_remote_copy(
            src_ref=chunk.at[i, other], dst_ref=dgot.at[s, i], send_sem=d_s.at[s, i], recv_sem=d_r.at[s, i],
            device_id=device(0, 0, 0, other), device_id_type=MESH,
        )

    def down(rows, s, i):
        with jax.named_scope("down"):
            column = pl.multiple_of(((y + ORDER[i]) % RING) * 2 * CHUNK, CHUNK)
            value = jnp.dot(hid[:, rows, :].reshape(BATCH, HID), wd[:, pl.ds(column, 2 * CHUNK)], preferred_element_type=f32).astype(bf16)
            chunk[i, 0] = value[:, :CHUNK]
            chunk[i, 1] = value[:, CHUNK:]
            d_copy(s, i).start()

    def join(b, s, i):
        with jax.named_scope("join"):
            d_copy(s, i).wait()
        mine[b % 4, i] = chunk[i, c] + dgot[s, i]

    def backs(b, rows, hook):
        s = b % 2
        down(rows, s, 0)

        @pl.when(s == 1)
        def _():
            join(b + 3, 0, 3)

        hook(3)
        down(rows, s, 1)
        down(rows, s, 2)
        join(b, s, 0)
        hook(4)
        down(rows, s, 3)
        join(b, s, 1)
        hook(5)
        join(b, s, 2)
        hook(6)

    def fact_copies(stage):
        if stage == 0:
            for d in (2, 1, 3):
                push(("fx", d), facts.at[me], device(0, d, 0, c), len(IDS), 1)
        else:
            for d in (2, 1, 3):
                push(("fz", d), facts.at[pl.ds(z * RING, RING)], device(d, 0, 0, c), len(IDS) + 1, 1)

    def fact_waits(stage):
        pull(facts.at[pl.ds(0, 12 if stage else 3)], len(IDS) + stage)

    finish(fact_loads)
    lifted = jnp.exp(score_buf[...])
    gate_values = (lifted / jnp.sum(lifted, axis=0, keepdims=True)).astype(bf16).astype(f32)
    facts[me] = jnp.concatenate([ids_buf[...].astype(f32), gate_values], axis=0).astype(bf16)

    with jax.named_scope("enter"):
        pl.semaphore_wait(barrier, len(peers))
    with jax.named_scope("own"):
        finish(own_loads)
    parity = y % 2

    def own_view(dx, h, lanes):
        owner = z * RING + (x + dx) % RING
        rows = pl.ds(0, OWN) if h is None else pl.ds(64 * h, 64)
        return xall.at[c, owner, rows, pl.ds(pl.multiple_of(lanes * QUART, QUART), QUART)]

    own_ids = {}

    def own_send(axis, dx, h, step):
        key = ("x", (dx - step) % RING, h) if axis == "x" else ("y", dx)
        ident = own_ids.setdefault(key, len(IDS) + 2 + len(own_ids))
        to = device(0, step, 0, c) if axis == "x" else device(0, 0, step, c)
        push((axis, dx, h, step), own_view(dx, h, parity), to, ident)

    def own_got(axis, dx, h):
        if axis == "x":
            pull(own_view(dx, h, parity), own_ids["x", dx, h])
        else:
            pull(own_view(dx, None, 1 - parity), own_ids["y", dx])

    def sideways(dx, h):
        own_send("y", dx, h, (1, 3)[h])

    fact_copies(0)
    own_send("x", 0, 0, 1)
    own_send("x", 0, 1, 3)
    own_send("x", 0, 1, 1)
    own_send("x", 0, 0, 3)
    spread(1, True, 0, 0)
    fact_waits(0)
    fact_copies(1)
    spread(0, False, 0, 0)

    weight_loads = [load(wg_in, wg), load(wu_in, wu), load(wd_in, wd)]
    with jax.named_scope("ox1"):
        own_got("x", 3, 0)
        own_send("x", 3, 0, 1)
        sideways(3, 0)
        own_got("x", 1, 1)
        own_send("x", 1, 1, 3)
        sideways(1, 1)
    finish(weight_loads[:2])
    gates(z)
    hidden_owners((0,), 0)
    with jax.named_scope("ox2"):
        own_got("x", 3, 1)
        sideways(3, 1)
        own_got("x", 1, 0)
        sideways(1, 0)
    with jax.named_scope("bz"):
        arrive(1, True, 3, 0)
        arrive(1, True, 1, 0)
    with jax.named_scope("ox3"):
        own_got("x", 2, 0)
        sideways(2, 0)
        own_got("x", 2, 1)
        sideways(2, 1)
        spread(1, False, 1, 0)
        spread(1, False, 3, 0)
    with jax.named_scope("fz"):
        fact_waits(1)
    hidden_owners((0,), 1)
    hidden_owners((0,), 2)
    for dx in (3, 1, 2):
        with jax.named_scope("oy%d" % dx):
            own_got("y", dx, 0)
            spread(0, False, 0, dx)
            pair(0, 0, dx)
            pair(1, 0, dx)
        if dx != 2:
            gates((z + dx) % RING)
    with jax.named_scope("pairs"):
        pairs(0)
    finish(weight_loads[2:])

    def a(dz, dx):
        return lambda: arrive(0, False, dz, dx)

    def bb(dz, dx):
        return lambda: arrive(1, dx == 0, dz, dx)

    def run(f, *args):
        return lambda: f(*args)

    def xf(b, i):
        return run(x_first, b, i)

    plan = {
        (0, 0): [a(1, 0), a(3, 0)],
        (0, 2): [bb(1, 3), bb(1, 1)],
        (0, 4): [a(3, 3), a(1, 3)],
        (1, 3): [a(3, 1), a(1, 1), bb(3, 3), bb(3, 1)],
        (1, 4): [bb(2, 0), run(spread, 1, False, 2, 0)],
        (2, 0): [run(gates, (z + 2) % RING), a(1, 2), a(3, 2), bb(1, 2), run(pairs, 1), run(y_second, 0)],
        (2, 1): [run(y_second, 1)],
        (2, 4): [run(y_third, 0)],
        (3, 0): [bb(3, 2)],
        (2, 6): [bb(2, 3), bb(2, 1)],
        (3, 6): [run(y_mid, 0), run(y_third, 1)],
        (4, 0): [run(pairs, 3)],
        (4, 3): [a(2, 0), a(2, 3), a(2, 1), bb(2, 2), a(2, 2), run(y_mid, 1)],
        (5, 3): [run(y_final, 0)],
        (5, 6): [run(y_final, 1)],
        (6, 0): [run(pairs, 2)],
    }

    def later(step, point, work):
        if step < STEPS:
            plan.setdefault((step, point), []).append(work)

    for b in range(STEPS):
        if b % 2 == 0:
            stages = (
                (2, 1, y_second), (2, 1, x_second), (2, 4, y_third), (2, 4, x_third),
                (3, 6, y_mid), (3, 6, x_mid), (4, 2, y_final), (4, 2, x_final),
            )
        else:
            stages = (
                (1, 2, y_second), (1, 3, x_second), (1, 6, y_third), (2, 4, x_third),
                (3, 1, y_mid), (3, 2, x_mid), (3, 3, y_final), (3, 4, x_final),
            )
        if b % 2:
            stages = tuple(((2, 6, x_third) if work is x_third else (lag, point, work)) for lag, point, work in stages)
        if b == 2:
            stages = tuple(((2, 2, x_second) if work is x_second else (lag, point, work)) for lag, point, work in stages)
        if b >= STEPS - 4:
            stages = tuple(item for item in stages if item[2] not in (y_mid, x_mid))
        for lag, point, work in stages:
            if b > 1:
                later(b + lag, point, run(work, b))
    later(STEPS - 1, 6, run(y_second, STEPS - 2))
    for b in range(STEPS):
        later(b, 4, run(y_first, b))
        if b > 1:
            later(b, 5, run(x_first, b, 0))
            if b % 2 == 0:
                later(b + 1, 3, run(x_first, b, 1))
            else:
                plan.setdefault((b + 1, 1), []).insert(0, run(x_first, b, 1))

    def batch(b, carry):
        def hook(point):
            for value in range(STEPS):
                work = plan.get((value, point), [])
                if work:

                    @pl.when(b == value)
                    def _():
                        with jax.named_scope("hook%d" % point):
                            for item in work:
                                item()

        zz = (z + batch_z(b // 2)) % RING
        rows = pl.ds(pl.multiple_of((b % 2) * HALF, HALF), HALF)
        hook(0)

        for i in range(HID // TILE):

            @pl.when(b == 0)
            def _():
                hidden_owners((3, 1, 2), i)

            @pl.when((b % 2 == 0) & (b > 0))
            def _():
                hidden_row(zz, i)
                if i == 0:
                    join(b + 3, 1, 3)

            if i < 2:
                hook(1 + i)
        backs(b, rows, hook)
        return carry

    lax.fori_loop(0, STEPS, batch, 0)
    join(STEPS - 1, (STEPS - 1) % 2, 3)
    final = STEPS - 1
    x_first(final, 1)
    x_second(final - 1)
    y_second(final)
    y_final(final - 3)
    x_final(final - 3)
    x_second(final)
    y_third(final - 1)
    x_third(final - 1)
    y_final(final - 2)
    x_final(final - 2)
    y_third(final)
    x_third(final)
    for b in (final - 1, final):
        y_final(b)
        x_final(b)
    with jax.named_scope("last"):
        for part, ref in enumerate((zy, zx)):
            for h in range(2):
                rows, lanes = pl.ds(h * HALF, HALF), pl.ds(part * LANES, LANES)
                total = kept[rows, lanes]
                for b in range(2 + h, STEPS, 2):
                    z_copy(b, part).wait()
                    total = total + ref[b - 2].astype(f32)
                out[rows, lanes] = total.astype(bf16)
    with jax.named_scope("leave"):
        block = OWN * QUART
        small = sum(size for key, size in sent.items() if key[0] in ("fx", "fz"))
        blocks = (sum(sent.values()) - small) // block
        assert blocks * block + small == sum(sent.values())
        assert blocks == 60 and small == 15 * INFO * OWN
        for group, ref in enumerate((xall.at[:, pl.ds(0, 15)], facts.at[pl.ds(0, 15)])):
            pltpu.make_async_remote_copy(
                src_ref=ref, dst_ref=ref, send_sem=gsem.at[group], recv_sem=rsem.at[0],
                device_id=device(0, 0, 0, other), device_id_type=MESH,
            ).wait_send()


def local(tokens, scores, expert_ids, gate_weight, up_weight, down_weight):
    weights = [w.reshape(HID, WIDTH) for w in (gate_weight, up_weight, down_weight)]
    dma = pltpu.SemaphoreType.DMA
    count = len(IDS)
    scratch = [
        (HID, WIDTH), (HID, WIDTH), (HID, WIDTH),
        (RING, OWN, HID), (RING * RING, OWN, HID),
        (4, 4, BATCH, CHUNK), (4, 2, BATCH, CHUNK), (2, 4, BATCH, CHUNK),
        (2, 2, 128, CHUNK), (6, 2, 128, LANES),
        (2, 2, BATCH, CHUNK), (6, 2, BATCH, LANES),
        (2, BATCH, CHUNK), (6, BATCH, LANES),
        (2, 2, 32, CHUNK), (6, 2, 32, LANES), (2, 2, HALF, CHUNK), (6, 2, HALF, LANES), (4, 3, HALF, LANES),
        (6, 2, 4, 32, LANES), (6, 2, 4, HALF, LANES),
        (6, 4, HALF, LANES), (6, 2, 32, LANES), (6, 2, HALF, LANES), (4, 3, HALF, LANES),
    ]
    return pl.pallas_call(
        kernel,
        out_shape=jax.ShapeDtypeStruct((OWN, CHUNK), bf16),
        in_specs=[pl.BlockSpec(memory_space=pl.ANY)] * 6,
        out_specs=pl.BlockSpec(memory_space=pltpu.VMEM),
        scratch_shapes=[
            pltpu.VMEM((2, 16, OWN, 2 * QUART), bf16), pltpu.VMEM((16, INFO, OWN), bf16),
            pltpu.VMEM((TOP, OWN), f32), pltpu.VMEM((TOP, OWN), jnp.int32),
        ]
        + [pltpu.VMEM(shape, bf16) for shape in scratch]
        + [pltpu.VMEM((OWN, CHUNK), f32)]
        + [pltpu.VMEM((6, HALF, LANES), bf16)] * 4
        + [dma((9,)), dma((2,)), dma((count + 11,)), dma((2, 4)), dma((2, 4)), dma((108,)), dma((108,))],
        compiler_params=pltpu.CompilerParams(
            collective_id=0, has_side_effects=True, vmem_limit_bytes=67043328
        ),
    )(tokens, scores.T, expert_ids.T, *weights)


def solution(mesh):
    in_specs = (
        P("expert", None),
        P("expert", None),
        P("expert", None),
        P("expert", "tensor", None),
        P("expert", "tensor", None),
        P("expert", "tensor", None),
    )
    out_specs = P("expert", "tensor")
    return jax.shard_map(local, mesh=mesh, in_specs=in_specs, out_specs=out_specs, check_vma=False)
```
